256 devices in a mesh: kx: 16 (over y_lo, x, core), ky: 16 (over y_hi, z).
Axes of the slice: x: 4, y: 4 (y_hi: 2, y_lo: 2; y = y_hi * 2 + y_lo), z: 8, core: 2. Of those that a mesh axis runs over, the one named last changes fastest.
Arguments:
- coeffs: bfloat16 [16, 16, 2, 36, 128, 256], P('kx', 'ky'), may hold values from -1 to 1, as said below
- bands: int32 [32], replicated, may hold values from 0 to 35, as said below
- umklapp: int32 [2, 2], replicated, may hold values from -3 to 3
Outputs:
- flux: float32 [16, 16, 2], P('kx', 'ky')
- links: float32 [16, 16, 3, 2], P('kx', 'ky')
The draws below stay inside these ranges and needn't reach their ends.
Inputs may be any that keep to these rules, and one draw needn't show every extreme that they name: 32 different indices of stored bands. `coeffs`: coefficients of order 1 / sqrt(32768); link matrices between neighbouring k-points stay close enough to unitary that elimination without row exchanges has pivots of magnitude near one.
All inputs are finite; a program needn't handle non-finite values.
Results may differ from the reference program's by a relative error of at most 0.0003.
Values may be sent and summed in bfloat16 or wider, within the bound.
A program may use at most 128 MiB of HBM per device.

```python
import math
import jax
import jax.numpy as jnp
from jax import lax

GX = 128
GY = 256
NBAND = 32
NSTORE = 36
NKX = 16
NKY = 16


def draw_coeffs(key, part):
    gsize = GX * GY
    key_modes, key_mix, key_noise = jax.random.split(jax.random.fold_in(key, 11), 3)
    modes = jax.random.permutation(key_modes, gsize)[:NSTORE]
    freq_x = (modes // GY).astype(jnp.float32)
    freq_y = (modes % GY).astype(jnp.float32)
    grid_x = jnp.arange(GX, dtype=jnp.float32)
    grid_y = jnp.arange(GY, dtype=jnp.float32)
    phase = 2.0 * math.pi * (freq_x[:, None, None] * grid_x[None, :, None] / GX + freq_y[:, None, None] * grid_y[None, None, :] / GY)
    scale_base = 1.0 / math.sqrt(gsize)
    base_real = jnp.cos(phase) * scale_base
    base_imag = jnp.sin(phase) * scale_base
    mixing = 0.08 * jax.random.uniform(key_mix, (NKX, NKY, 2, NSTORE, NSTORE), jnp.float32, -1.0, 1.0)
    mix_real = jnp.eye(NSTORE, dtype=jnp.float32) + mixing[:, :, 0]
    mix_imag = mixing[:, :, 1]
    field_real = jnp.einsum('abmn,mxy->abnxy', mix_real, base_real) - jnp.einsum('abmn,mxy->abnxy', mix_imag, base_imag)
    field_imag = jnp.einsum('abmn,mxy->abnxy', mix_real, base_imag) + jnp.einsum('abmn,mxy->abnxy', mix_imag, base_real)
    noise = 0.3 * scale_base * jax.random.normal(key_noise, (NKX, NKY, 2, NSTORE, GX, GY), jnp.float32)
    return (jnp.stack([field_real, field_imag], axis=2) + noise).astype(jnp.bfloat16)


def draw_bands(key, part):
    return jax.random.permutation(jax.random.fold_in(key, 23), NSTORE)[:NBAND].astype(jnp.int32)


def touch_ends(values, rng, least, high):
    index_at = [jax.random.randint(jax.random.fold_in(rng, axis), (), 0, length) for axis, length in enumerate(values.shape)]
    main_axis = values.shape.index(max(values.shape))
    neighbour = index_at[:main_axis] + [(index_at[main_axis] + 1) % values.shape[main_axis]] + index_at[main_axis + 1:]
    return values.at[tuple(index_at)].set(least).at[tuple(neighbour)].set(high)


def setup_inputs(seed: int = 0) -> dict:
    seeds = jax.random.split(jax.random.key(seed), 4)
    return {
        "coeffs": draw_coeffs(jax.random.fold_in(seeds[3], 71), 0),
        "bands": draw_bands(jax.random.fold_in(seeds[3], 71), 0),
        "umklapp": touch_ends(jax.random.randint(seeds[2], (2, 2), -3, 4), jax.random.fold_in(seeds[2], 1), -3, 3).astype(jnp.int32),
    }


def correlation(left_block, right_block):
    count = left_block.shape[1]
    left_rows = left_block.reshape(2 * count, -1)
    right_rows = right_block.reshape(2 * count, -1)
    square = lax.dot_general(left_rows, right_rows, (((1,), (1,)), ((), ())), preferred_element_type=jnp.float32)
    real_part = square[:count, :count] + square[count:, count:]
    imag_part = square[:count, count:] - square[count:, :count]
    return (real_part, imag_part)

def det_units(real_stack, imag_stack):
    count = real_stack.shape[1]
    places = jnp.arange(count, dtype=jnp.int32)

    def elimination(pivot_row, carry):
        work_real, work_imag, unit_real, unit_imag = carry
        pivot_real = work_real[:, pivot_row, pivot_row]
        pivot_imag = work_imag[:, pivot_row, pivot_row]
        square_mag = pivot_real * pivot_real + pivot_imag * pivot_imag
        inverse_real = pivot_real / square_mag
        inverse_imag = -pivot_imag / square_mag
        column_real = work_real[:, :, pivot_row]
        column_imag = work_imag[:, :, pivot_row]
        below = (places > pivot_row).astype(jnp.float32)[None, :]
        factor_real = (column_real * inverse_real[:, None] - column_imag * inverse_imag[:, None]) * below
        factor_imag = (column_real * inverse_imag[:, None] + column_imag * inverse_real[:, None]) * below
        row_real = work_real[:, pivot_row, :]
        row_imag = work_imag[:, pivot_row, :]
        work_real = work_real - (factor_real[:, :, None] * row_real[:, None, :] - factor_imag[:, :, None] * row_imag[:, None, :])
        work_imag = work_imag - (factor_real[:, :, None] * row_imag[:, None, :] + factor_imag[:, :, None] * row_real[:, None, :])
        magnitude = jnp.sqrt(square_mag)
        next_real = (unit_real * pivot_real - unit_imag * pivot_imag) / magnitude
        next_imag = (unit_real * pivot_imag + unit_imag * pivot_real) / magnitude
        return (work_real, work_imag, next_real, next_imag)
    batch = real_stack.shape[0]
    start = (real_stack, imag_stack, jnp.ones((batch,), jnp.float32), jnp.zeros((batch,), jnp.float32))
    result = lax.fori_loop(0, count, elimination, start)
    return jnp.stack([result[2], result[3]], axis=-1)

def rolled(block, offset):
    return jnp.roll(block, (offset[0], offset[1]), axis=(2, 3))

def times(first, second):
    return jnp.stack([first[..., 0] * second[..., 0] - first[..., 1] * second[..., 1], first[..., 0] * second[..., 1] + first[..., 1] * second[..., 0]], axis=-1)

def conjugate(value):
    return jnp.stack([value[..., 0], -value[..., 1]], axis=-1)

def reference(coeffs, bands, umklapp):

    def one_point(flat):
        row = flat // NKY
        column = flat % NKY
        next_row = (row + 1) % NKX
        next_column = (column + 1) % NKY
        own_block = jnp.take(coeffs[row, column], bands, axis=1)
        right_block = jnp.take(coeffs[next_row, column], bands, axis=1)
        upper_block = jnp.take(coeffs[row, next_column], bands, axis=1)
        corner_block = jnp.take(coeffs[next_row, next_column], bands, axis=1)
        shift_x = jnp.where(row == NKX - 1, umklapp[0], jnp.zeros((2,), jnp.int32))
        shift_y = jnp.where(column == NKY - 1, umklapp[1], jnp.zeros((2,), jnp.int32))
        first_real, first_imag = correlation(own_block, rolled(right_block, shift_x))
        second_real, second_imag = correlation(own_block, rolled(upper_block, shift_y))
        third_real, third_imag = correlation(own_block, rolled(corner_block, shift_x + shift_y))
        real_stack = jnp.stack([first_real, second_real, third_real])
        imag_stack = jnp.stack([first_imag, second_imag, third_imag])
        return det_units(real_stack, imag_stack)
    links = lax.map(one_point, jnp.arange(NKX * NKY, dtype=jnp.int32)).reshape(NKX, NKY, 3, 2)
    along_x = links[:, :, 0]
    along_y = links[:, :, 1]
    along_d = links[:, :, 2]
    y_next = jnp.roll(along_y, -1, axis=0)
    x_next = jnp.roll(along_x, -1, axis=1)
    first = times(times(along_x, y_next), conjugate(along_d))
    second = times(times(along_d, conjugate(x_next)), conjugate(along_y))
    flux = jnp.stack([jnp.arctan2(first[..., 1], first[..., 0]), jnp.arctan2(second[..., 1], second[..., 0])], axis=-1)
    return (flux, links)
```

```python
import functools

import jax
import jax.numpy as jnp
from jax import lax
from jax.experimental import pallas as pl
from jax.experimental.pallas import tpu as pltpu
from jax.sharding import PartitionSpec as P

MESH = pl.DeviceIdType.MESH
NB = 32
ROWS = 2 * NB
GX = 128
GY = 256
HALF = GX // 2
EXTRA = 3
CHUNK = 8
NCHUNK = HALF // CHUNK
TILE = 16
F32 = jnp.float32
CONTRACT = (((1,), (1,)), ((), ()))


def dot(a, b):
    return lax.dot_general(a, b, CONTRACT, preferred_element_type=F32)


def complex_parts(square):
    real = square[:NB, :NB] + square[NB:, NB:]
    imag = square[:NB, NB:] - square[NB:, :NB]
    return real, imag


def eliminate(wr, wi):
    lane = lax.broadcasted_iota(jnp.int32, (NB, 128), 1)
    row_id = lax.broadcasted_iota(jnp.int32, (NB, 128), 0)
    base = (lane // NB) * NB
    pivots_r, pivots_i = [], []
    for k in range(NB):
        where = base + k
        col_r = jnp.take_along_axis(wr, where, axis=1)
        col_i = jnp.take_along_axis(wi, where, axis=1)
        pr = col_r[k : k + 1]
        pi = col_i[k : k + 1]
        pivots_r.append(pr)
        pivots_i.append(pi)
        if k == NB - 1:
            break
        mag = pr * pr + pi * pi
        inv_r = pr / mag
        inv_i = -pi / mag
        below = row_id > k
        fr = jnp.where(below, col_r * inv_r - col_i * inv_i, 0.0)
        fi = jnp.where(below, col_r * inv_i + col_i * inv_r, 0.0)
        row_r = wr[k : k + 1]
        row_i = wi[k : k + 1]
        wr, wi = (
            wr - (fr * row_r - fi * row_i),
            wi - (fr * row_i + fi * row_r),
        )
    pr = jnp.concatenate(pivots_r, axis=0)
    pi = jnp.concatenate(pivots_i, axis=0)
    mag = jnp.sqrt(pr * pr + pi * pi)
    ur = pr / mag
    ui = pi / mag
    n = NB
    while n > 1:
        n //= 2
        ar, ai, br, bi = ur[:n], ui[:n], ur[n:], ui[n:]
        ur, ui = ar * br - ai * bi, ar * bi + ai * br
    return ur, ui


def kernel(
    bands, umk, coeffs, out,
    cv, u, zm, zp, xp, xm, szm, szp, sxp, sxm, wb, xb,
    acc_a, acc_b, acc_d, left_src, left_dst, down_src, down_dst,
    unit, unit_x, unit_y,
    load_sem, send_sem, recv_sem, ez_sem, part_sem, unit_sem,
):
    i = lax.axis_index("kx")
    j = lax.axis_index("ky")
    ni = lax.axis_size("kx")
    nj = lax.axis_size("ky")
    right = (lax.rem(i + 1, ni), j)
    left = (lax.rem(i + ni - 1, ni), j)
    up = (i, lax.rem(j + 1, nj))
    down = (i, lax.rem(j + nj - 1, nj))
    x_edge = i == ni - 1
    y_edge = j == 0
    edge = jnp.logical_or(x_edge, y_edge)

    def load(t):
        rows = pl.ds(t * TILE, TILE)
        return pltpu.make_async_copy(coeffs.at[:, :, rows, :], cv[t], load_sem.at[t])

    half_tiles = HALF // TILE
    for t in range(half_tiles):
        load(t).start()
        load(t + half_tiles).start()

    barrier = pltpu.get_barrier_semaphore()
    for device in (right, left, up, down):
        pl.semaphore_signal(barrier, inc=1, device_id=device, device_id_type=MESH)

    zero = jnp.int32(0)
    ax = jnp.where(x_edge, umk[0, 0], zero)
    bx = jnp.where(x_edge, umk[0, 1], zero)
    ay = jnp.where(y_edge, umk[1, 0], zero)
    by = jnp.where(y_edge, umk[1, 1], zero)

    acc_a[...] = jnp.zeros_like(acc_a)
    acc_b[...] = jnp.zeros_like(acc_b)
    acc_d[...] = jnp.zeros_like(acc_d)

    def remote(src, dst, stream, c, device):
        return pltpu.make_async_remote_copy(
            src_ref=src, dst_ref=dst, send_sem=send_sem.at[stream, c],
            recv_sem=recv_sem.at[stream, c], device_id=device, device_id_type=MESH,
        )

    def stream_copy(stream, c, special):
        low = pl.ds(c * CHUNK, CHUNK)
        high = pl.ds(HALF + c * CHUNK, CHUNK)
        own, src, dst, device = (
            (low, szm, zm, down),
            (high, szp, zp, up),
            (low, sxp, xp, right),
            (high, sxm, xm, left),
        )[stream]
        source = src.at[low] if special else u.at[own]
        return remote(source, dst.at[low], stream, c, device)

    need = (y_edge, x_edge, x_edge, y_edge)

    def gather(t):
        rows = pl.ds(t * TILE, TILE)
        parts = [cv[t][r, bands[b]] for r in range(2) for b in range(NB)]
        u[rows] = jnp.swapaxes(jnp.stack(parts, axis=0), 0, 1)

    for t in range(half_tiles):
        load(t).wait()
        gather(t)
        load(t + half_tiles).wait()
        gather(t + half_tiles)
        if t == 0:
            pl.semaphore_wait(barrier, 4)
        for c in range(t * TILE // CHUNK, (t + 1) * TILE // CHUNK):
            for stream in range(4):

                @pl.when(jnp.logical_not(need[stream]))
                def _(stream=stream, c=c):
                    stream_copy(stream, c, False).start()

    def build(dst, count, first, dp, dq):
        shift = lax.rem(GY - dq, GY)

        @pl.loop(0, count)
        def _(p):
            row = lax.rem(first + p + dp + GX, GX)
            dst[p] = pltpu.roll(u[row], shift, 1)

    def build_extra(dst, forward, dq):
        shift = lax.rem(GY - dq, GY)
        for e in range(EXTRA):
            row = jnp.where(forward, e, HALF - EXTRA + e)
            dst[HALF + e] = pltpu.roll(u[row], shift, 1)

    def extra(stream, src, dst, device):
        rows = pl.ds(HALF, EXTRA)
        return pltpu.make_async_remote_copy(
            src_ref=src.at[rows], dst_ref=dst.at[rows], send_sem=ez_sem.at[0, stream],
            recv_sem=ez_sem.at[1, stream], device_id=device, device_id_type=MESH,
        )

    @pl.when(y_edge)
    def _():
        build(szm, HALF, 0, -ay, -by)
        for c in range(NCHUNK):
            stream_copy(0, c, True).start()

    @pl.when(x_edge)
    def _():
        build(szp, HALF, HALF, 0, bx)
        build_extra(szp, ax > 0, bx)
        extra(0, szp, zp, up).start()
        for c in range(NCHUNK):
            stream_copy(1, c, True).start()
        build(sxp, HALF, 0, ax, bx)
        for c in range(NCHUNK):
            stream_copy(2, c, True).start()

    @pl.when(y_edge)
    def _():
        build(sxm, HALF, HALF, 0, -by)
        build_extra(sxm, ay < 0, -by)
        extra(1, sxm, xm, left).start()
        for c in range(NCHUNK):
            stream_copy(3, c, True).start()

    build(wb, HALF, HALF, -ay, bx - by)
    build(xb, HALF, HALF, ax, bx - by)

    @pl.loop(0, NCHUNK)
    def _(c):
        for stream in range(4):
            stream_copy(stream, c, False).wait_recv()
        first = c * CHUNK
        a = None
        b = None
        for q in range(CHUNK):
            p = first + q
            own = u[p]
            lhs = jnp.concatenate([own, xp[p]], axis=0)
            rhs = jnp.concatenate([zm[p], own], axis=0)
            term = dot(lhs, rhs)
            a = term if a is None else a + term
            lhs = jnp.concatenate([zp[p], xb[p]], axis=0)
            rhs = jnp.concatenate([wb[p], xm[p]], axis=0)
            term = dot(lhs, rhs)
            b = term if b is None else b + term
        acc_a[...] += a
        acc_b[...] += b

    acc_d[...] = acc_b[:ROWS, ROWS:]

    @pl.when(x_edge)
    def _():
        extra(0, szp, zp, up).wait_recv()

    @pl.when(y_edge)
    def _():
        extra(1, sxm, xm, left).wait_recv()

    @pl.when(edge)
    def _():
        acc_d[...] = jnp.zeros_like(acc_d)

        @pl.loop(0, HALF // 8)
        def _(c):
            total = None
            for q in range(8):
                s = c * 8 + q + ax
                t = c * 8 + q - ay
                s = jnp.where(s < 0, s + HALF + EXTRA, s)
                t = jnp.where(t < 0, t + HALF + EXTRA, t)
                term = dot(zp[s], xm[t])
                total = term if total is None else total + term
            acc_d[...] += total

    a = acc_a[...]
    b = acc_b[...]
    d_low = complex_parts(a[ROWS:, :ROWS])
    x_low = complex_parts(a[ROWS:, ROWS:])
    y_low = complex_parts(a[:ROWS, :ROWS])
    y_high = complex_parts(b[:ROWS, :ROWS])
    x_high = complex_parts(b[ROWS:, ROWS:])
    d_high = complex_parts(acc_d[...])
    none = jnp.zeros((NB, NB), F32)

    for part in range(2):
        rows = pl.ds(part * NB, NB)
        left_src[rows, :] = jnp.concatenate([x_low[part], none, d_low[part], none], axis=1)
        down_src[rows, :] = jnp.concatenate([none, y_high[part], d_high[part], none], axis=1)

    def part_copy(which):
        src, dst, device = ((left_src, left_dst, left), (down_src, down_dst, down))[which]
        return pltpu.make_async_remote_copy(
            src_ref=src, dst_ref=dst, send_sem=part_sem.at[0, which],
            recv_sem=part_sem.at[1, which], device_id=device, device_id_type=MESH,
        )

    for which in range(2):
        part_copy(which).start()
    own = [
        jnp.concatenate([x_high[part], y_low[part], none, none], axis=1) for part in range(2)
    ]
    for which in range(2):
        part_copy(which).wait_recv()
    wr, wi = (
        own[part] + left_dst[pl.ds(part * NB, NB), :] + down_dst[pl.ds(part * NB, NB), :]
        for part in range(2)
    )
    lane = lax.broadcasted_iota(jnp.int32, (NB, 128), 1)
    unused = lane >= 3 * NB
    wr = jnp.where(unused, 1.0, wr)
    ur, ui = eliminate(wr, wi)
    unit[0:1, :] = ur
    unit[1:2, :] = ui

    def unit_copy(which):
        dst, device = ((unit_x, left), (unit_y, down))[which]
        return pltpu.make_async_remote_copy(
            src_ref=unit, dst_ref=dst, send_sem=unit_sem.at[0, which],
            recv_sem=unit_sem.at[1, which], device_id=device, device_id_type=MESH,
        )

    for which in range(2):
        unit_copy(which).start()
    for which in range(2):
        unit_copy(which).wait_recv()
    out[0:2, :] = unit[0:2, :]
    out[2:4, :] = unit_x[0:2, :]
    out[4:6, :] = unit_y[0:2, :]
    out[6:8, :] = jnp.zeros((2, 128), F32)

    @pl.loop(0, NCHUNK)
    def _(c):
        for stream in range(4):
            stream_copy(stream, c, False).wait_send()

    @pl.when(x_edge)
    def _():
        extra(0, szp, zp, up).wait_send()

    @pl.when(y_edge)
    def _():
        extra(1, sxm, xm, left).wait_send()

    for which in range(2):
        part_copy(which).wait_send()
        unit_copy(which).wait_send()


def times(a, b):
    return a[0] * b[0] - a[1] * b[1], a[0] * b[1] + a[1] * b[0]


def conjugate(a):
    return a[0], -a[1]


def per_device(coeffs, bands, umklapp):
    bf16 = jnp.bfloat16
    half = pltpu.VMEM((HALF, ROWS, GY), bf16)
    longer = pltpu.VMEM((HALF + EXTRA, ROWS, GY), bf16)
    table = pl.pallas_call(
        kernel,
        out_shape=jax.ShapeDtypeStruct((8, 128), F32),
        in_specs=[
            pl.BlockSpec(memory_space=pltpu.SMEM),
            pl.BlockSpec(memory_space=pltpu.SMEM),
            pl.BlockSpec(memory_space=pl.ANY),
        ],
        out_specs=pl.BlockSpec(memory_space=pltpu.VMEM),
        scratch_shapes=[
            [pltpu.VMEM((*coeffs.shape[2:4], TILE, GY), bf16)] * (GX // TILE),
            pltpu.VMEM((GX, ROWS, GY), bf16),
            half, longer, half, longer,
            half, longer, half, longer, half, half,
            pltpu.VMEM((2 * ROWS, 2 * ROWS), F32),
            pltpu.VMEM((2 * ROWS, 2 * ROWS), F32),
            pltpu.VMEM((ROWS, ROWS), F32),
            pltpu.VMEM((ROWS, 128), F32),
            pltpu.VMEM((ROWS, 128), F32),
            pltpu.VMEM((ROWS, 128), F32),
            pltpu.VMEM((ROWS, 128), F32),
            pltpu.VMEM((8, 128), F32),
            pltpu.VMEM((8, 128), F32),
            pltpu.VMEM((8, 128), F32),
            pltpu.SemaphoreType.DMA((GX // TILE,)),
            pltpu.SemaphoreType.DMA((4, NCHUNK)),
            pltpu.SemaphoreType.DMA((4, NCHUNK)),
            pltpu.SemaphoreType.DMA((2, 2)),
            pltpu.SemaphoreType.DMA((2, 2)),
            pltpu.SemaphoreType.DMA((2, 2)),
        ],
        compiler_params=pltpu.CompilerParams(
            collective_id=0, has_side_effects=True, vmem_limit_bytes=56 << 20
        ),
    )(bands, umklapp, coeffs[0, 0])

    def link(row, which):
        return table[row, which * NB], table[row + 1, which * NB]

    along_x, along_y, along_d = (link(0, which) for which in range(3))
    y_next = link(2, 1)
    x_next = link(4, 0)
    first = times(times(along_x, y_next), conjugate(along_d))
    second = times(times(along_d, conjugate(x_next)), conjugate(along_y))
    flux = jnp.stack([jnp.arctan2(first[1], first[0]), jnp.arctan2(second[1], second[0])])
    links = jnp.stack([*along_x, *along_y, *along_d])
    return flux.reshape(1, 1, 2), links.reshape(1, 1, 3, 2)


def solution(mesh):
    in_specs = (P("kx", "ky", None, None, None, None), P(), P())
    out_specs = (P("kx", "ky", None), P("kx", "ky", None, None))
    return jax.shard_map(
        per_device, mesh=mesh, in_specs=in_specs, out_specs=out_specs, check_vma=False
    )
```

```python
import functools

import jax
import jax.numpy as jnp
from jax import lax
from jax.experimental import pallas as pl
from jax.experimental.pallas import tpu as pltpu
from jax.sharding import PartitionSpec as P

MESH = pl.DeviceIdType.MESH
NB = 32
ROWS = 2 * NB
GX = 128
GY = 256
HALF = GX // 2
EXTRA = 3
CHUNK = 8
NCHUNK = HALF // CHUNK
TILE = 16
F32 = jnp.float32
CONTRACT = (((1,), (1,)), ((), ()))


def dot(a, b):
    return lax.dot_general(a, b, CONTRACT, preferred_element_type=F32)


def complex_parts(square):
    real = square[:NB, :NB] + square[NB:, NB:]
    imag = square[:NB, NB:] - square[NB:, :NB]
    return real, imag


def times(a, b):
    return a[0] * b[0] - a[1] * b[1], a[0] * b[1] + a[1] * b[0]


def conjugate(a):
    return a[0], -a[1]


def eliminate(wr, wi):
    lane = lax.broadcasted_iota(jnp.int32, (NB, 128), 1)
    row_id = lax.broadcasted_iota(jnp.int32, (NB, 128), 0)
    base = (lane // NB) * NB
    pivots_r, pivots_i = [], []
    for k in range(NB):
        where = base + k
        col_r = jnp.take_along_axis(wr, where, axis=1)
        col_i = jnp.take_along_axis(wi, where, axis=1)
        pr = col_r[k : k + 1]
        pi = col_i[k : k + 1]
        pivots_r.append(pr)
        pivots_i.append(pi)
        if k == NB - 1:
            break
        mag = pr * pr + pi * pi
        inv_r = pr / mag
        inv_i = -pi / mag
        below = row_id > k
        fr = jnp.where(below, col_r * inv_r - col_i * inv_i, 0.0)
        fi = jnp.where(below, col_r * inv_i + col_i * inv_r, 0.0)
        row_r = wr[k : k + 1]
        row_i = wi[k : k + 1]
        wr, wi = (
            wr - (fr * row_r - fi * row_i),
            wi - (fr * row_i + fi * row_r),
        )
    pr = jnp.concatenate(pivots_r, axis=0)
    pi = jnp.concatenate(pivots_i, axis=0)
    mag = jnp.sqrt(pr * pr + pi * pi)
    ur = pr / mag
    ui = pi / mag
    n = NB
    while n > 1:
        n //= 2
        ar, ai, br, bi = ur[:n], ui[:n], ur[n:], ui[n:]
        ur, ui = ar * br - ai * bi, ar * bi + ai * br
    return ur, ui


def kernel(
    bands, umk, coeffs, flux, links,
    cv, perm, u, zm, zp, xp, xm, szm, szp, sxp, sxm, wb, xb,
    acc_a, acc_b, acc_d, left_src, left_dst, down_src, down_dst,
    unit, unit_x, unit_y,
    load_sem, send_sem, recv_sem, ez_sem, part_sem, unit_sem,
):
    i = lax.axis_index("kx")
    j = lax.axis_index("ky")
    ni = lax.axis_size("kx")
    nj = lax.axis_size("ky")
    right = (lax.rem(i + 1, ni), j)
    left = (lax.rem(i + ni - 1, ni), j)
    up = (i, lax.rem(j + 1, nj))
    down = (i, lax.rem(j + nj - 1, nj))
    x_edge = i == ni - 1
    y_edge = j == 0
    edge = jnp.logical_or(x_edge, y_edge)

    def load(t):
        rows = pl.ds(t * TILE, TILE)
        return pltpu.make_async_copy(coeffs.at[:, :, rows, :], cv[t], load_sem.at[t])

    half_tiles = HALF // TILE
    for t in range(half_tiles):
        load(t).start()
        load(t + half_tiles).start()

    barrier = pltpu.get_barrier_semaphore()
    for device in (right, left, up, down):
        pl.semaphore_signal(barrier, inc=1, device_id=device, device_id_type=MESH)

    zero = jnp.int32(0)
    ax = jnp.where(x_edge, umk[0, 0], zero)
    bx = jnp.where(x_edge, umk[0, 1], zero)
    ay = jnp.where(y_edge, umk[1, 0], zero)
    by = jnp.where(y_edge, umk[1, 1], zero)

    size = TILE * TILE
    to = lax.broadcasted_iota(jnp.int32, (size, size), 0)
    take = lax.broadcasted_iota(jnp.int32, (size, size), 1)
    swap = (to % TILE) * TILE + to // TILE
    perm[...] = jnp.where(take == swap, 1.0, 0.0).astype(jnp.bfloat16)

    acc_a[...] = jnp.zeros_like(acc_a)
    acc_b[...] = jnp.zeros_like(acc_b)
    acc_d[...] = jnp.zeros_like(acc_d)

    def remote(src, dst, stream, c, device):
        return pltpu.make_async_remote_copy(
            src_ref=src, dst_ref=dst, send_sem=send_sem.at[stream, c],
            recv_sem=recv_sem.at[stream, c], device_id=device, device_id_type=MESH,
        )

    def stream_copy(stream, c, special):
        low = pl.ds(c * CHUNK, CHUNK)
        high = pl.ds(HALF + c * CHUNK, CHUNK)
        own, src, dst, device = (
            (low, szm, zm, down),
            (high, szp, zp, up),
            (low, sxp, xp, right),
            (high, sxm, xm, left),
        )[stream]
        source = src.at[low] if special else u.at[own]
        return remote(source, dst.at[low], stream, c, device)

    need = (y_edge, x_edge, x_edge, y_edge)

    def gather(t):
        rows = pl.ds(t * TILE, TILE)
        for g in range(ROWS // TILE):
            r, b = divmod(g * TILE, NB)
            parts = [cv[t][r, bands[b + e]] for e in range(TILE)]
            moved = jnp.dot(perm[...], jnp.concatenate(parts, axis=0), preferred_element_type=F32)
            moved = moved.astype(jnp.bfloat16).reshape(TILE, TILE, GY)
            u[rows, pl.ds(g * TILE, TILE), :] = moved

    for t in range(half_tiles):
        load(t).wait()
        gather(t)
        load(t + half_tiles).wait()
        gather(t + half_tiles)
        if t == 0:
            pl.semaphore_wait(barrier, 4)
        for c in range(t * TILE // CHUNK, (t + 1) * TILE // CHUNK):
            for stream in range(4):

                @pl.when(jnp.logical_not(need[stream]))
                def _(stream=stream, c=c):
                    stream_copy(stream, c, False).start()

    def build(dst, count, first, dp, dq):
        shift = lax.rem(GY - dq, GY)

        @pl.loop(0, count // 8)
        def _(c):
            for q in range(8):
                p = c * 8 + q
                row = lax.rem(first + p + dp + GX, GX)
                dst[p] = pltpu.roll(u[row], shift, 1)

    def build_extra(dst, forward, dq):
        shift = lax.rem(GY - dq, GY)
        for e in range(EXTRA):
            row = jnp.where(forward, e, HALF - EXTRA + e)
            dst[HALF + e] = pltpu.roll(u[row], shift, 1)

    def extra(stream, src, dst, device):
        rows = pl.ds(HALF, EXTRA)
        return pltpu.make_async_remote_copy(
            src_ref=src.at[rows], dst_ref=dst.at[rows], send_sem=ez_sem.at[0, stream],
            recv_sem=ez_sem.at[1, stream], device_id=device, device_id_type=MESH,
        )

    @pl.when(y_edge)
    def _():
        build(szm, HALF, 0, -ay, -by)
        for c in range(NCHUNK):
            stream_copy(0, c, True).start()

    @pl.when(x_edge)
    def _():
        build(szp, HALF, HALF, 0, bx)
        build_extra(szp, ax > 0, bx)
        extra(0, szp, zp, up).start()
        for c in range(NCHUNK):
            stream_copy(1, c, True).start()
        build(sxp, HALF, 0, ax, bx)
        for c in range(NCHUNK):
            stream_copy(2, c, True).start()

    @pl.when(y_edge)
    def _():
        build(sxm, HALF, HALF, 0, -by)
        build_extra(sxm, ay < 0, -by)
        extra(1, sxm, xm, left).start()
        for c in range(NCHUNK):
            stream_copy(3, c, True).start()

    build(wb, HALF, HALF, -ay, bx - by)
    build(xb, HALF, HALF, ax, bx - by)

    @pl.loop(0, NCHUNK)
    def _(c):
        for stream in range(4):
            stream_copy(stream, c, False).wait_recv()
        first = c * CHUNK
        a = None
        b = None
        for q in range(CHUNK):
            p = first + q
            own = u[p]
            lhs = jnp.concatenate([own, xp[p]], axis=0)
            rhs = jnp.concatenate([zm[p], own], axis=0)
            term = dot(lhs, rhs)
            a = term if a is None else a + term
            lhs = jnp.concatenate([zp[p], xb[p]], axis=0)
            rhs = jnp.concatenate([wb[p], xm[p]], axis=0)
            term = dot(lhs, rhs)
            b = term if b is None else b + term
        acc_a[...] += a
        acc_b[...] += b

    acc_d[...] = acc_b[:ROWS, ROWS:]

    @pl.when(x_edge)
    def _():
        extra(0, szp, zp, up).wait_recv()

    @pl.when(y_edge)
    def _():
        extra(1, sxm, xm, left).wait_recv()

    @pl.when(edge)
    def _():
        acc_d[...] = jnp.zeros_like(acc_d)

        @pl.loop(0, HALF // 8)
        def _(c):
            total = None
            for q in range(8):
                s = c * 8 + q + ax
                t = c * 8 + q - ay
                s = jnp.where(s < 0, s + HALF + EXTRA, s)
                t = jnp.where(t < 0, t + HALF + EXTRA, t)
                term = dot(zp[s], xm[t])
                total = term if total is None else total + term
            acc_d[...] += total

    a = acc_a[...]
    b = acc_b[...]
    d_low = complex_parts(a[ROWS:, :ROWS])
    x_low = complex_parts(a[ROWS:, ROWS:])
    y_low = complex_parts(a[:ROWS, :ROWS])
    y_high = complex_parts(b[:ROWS, :ROWS])
    x_high = complex_parts(b[ROWS:, ROWS:])
    d_high = complex_parts(acc_d[...])
    none = jnp.zeros((NB, NB), F32)

    for part in range(2):
        rows = pl.ds(part * NB, NB)
        left_src[rows, :] = jnp.concatenate([x_low[part], none, d_low[part], none], axis=1)
        down_src[rows, :] = jnp.concatenate([none, y_high[part], d_high[part], none], axis=1)

    def part_copy(which):
        src, dst, device = ((left_src, left_dst, left), (down_src, down_dst, down))[which]
        return pltpu.make_async_remote_copy(
            src_ref=src, dst_ref=dst, send_sem=part_sem.at[0, which],
            recv_sem=part_sem.at[1, which], device_id=device, device_id_type=MESH,
        )

    for which in range(2):
        part_copy(which).start()
    own = [
        jnp.concatenate([x_high[part], y_low[part], none, none], axis=1) for part in range(2)
    ]
    for which in range(2):
        part_copy(which).wait_recv()
    wr, wi = (
        own[part] + left_dst[pl.ds(part * NB, NB), :] + down_dst[pl.ds(part * NB, NB), :]
        for part in range(2)
    )
    lane = lax.broadcasted_iota(jnp.int32, (NB, 128), 1)
    unused = lane >= 3 * NB
    wr = jnp.where(unused, 1.0, wr)
    ur, ui = eliminate(wr, wi)
    unit[0:1, :] = ur
    unit[1:2, :] = ui

    def unit_copy(which):
        dst, device = ((unit_x, left), (unit_y, down))[which]
        return pltpu.make_async_remote_copy(
            src_ref=unit, dst_ref=dst, send_sem=unit_sem.at[0, which],
            recv_sem=unit_sem.at[1, which], device_id=device, device_id_type=MESH,
        )

    for which in range(2):
        unit_copy(which).start()
    for which in range(2):
        unit_copy(which).wait_recv()

    def group(ref, which):
        real, imag = ref[0:1, :], ref[1:2, :]
        if which:
            shift = 128 - which * NB
            real, imag = pltpu.roll(real, shift, 1), pltpu.roll(imag, shift, 1)
        return real, imag

    along_x, along_y, along_d = (group(unit, which) for which in range(3))
    y_next = group(unit_x, 1)
    x_next = group(unit_y, 0)
    first = times(times(along_x, y_next), conjugate(along_d))
    second = times(times(along_d, conjugate(x_next)), conjugate(along_y))
    is_real = lax.broadcasted_iota(jnp.int32, (1, 128), 1) == 0
    angle = jnp.arctan2(
        jnp.where(is_real, first[1], second[1]), jnp.where(is_real, first[0], second[0])
    )
    flux[0] = angle[:, :2]
    lane = lax.broadcasted_iota(jnp.int32, (1, 128), 1)
    for part in range(2):
        row = jnp.where(lane == 0, along_x[part], along_y[part])
        row = jnp.where(lane == 2, along_d[part], row)
        links[0, 0, part : part + 1, :] = row[:, :3]

    @pl.loop(0, NCHUNK)
    def _(c):
        for stream in range(4):
            stream_copy(stream, c, False).wait_send()

    @pl.when(x_edge)
    def _():
        extra(0, szp, zp, up).wait_send()

    @pl.when(y_edge)
    def _():
        extra(1, sxm, xm, left).wait_send()

    for which in range(2):
        part_copy(which).wait_send()
        unit_copy(which).wait_send()


def per_device(coeffs, bands, umklapp):
    bf16 = jnp.bfloat16
    half = pltpu.VMEM((HALF, ROWS, GY), bf16)
    longer = pltpu.VMEM((HALF + EXTRA, ROWS, GY), bf16)
    flux, links = pl.pallas_call(
        kernel,
        out_shape=(
            jax.ShapeDtypeStruct((1, 1, 2), F32),
            jax.ShapeDtypeStruct((1, 1, 2, 3), F32),
        ),
        in_specs=[
            pl.BlockSpec(memory_space=pltpu.SMEM),
            pl.BlockSpec(memory_space=pltpu.SMEM),
            pl.BlockSpec(memory_space=pl.ANY),
        ],
        out_specs=(pl.BlockSpec(memory_space=pltpu.VMEM),) * 2,
        scratch_shapes=[
            [pltpu.VMEM((*coeffs.shape[2:4], TILE, GY), bf16)] * (GX // TILE),
            pltpu.VMEM((TILE * TILE, TILE * TILE), bf16),
            pltpu.VMEM((GX, ROWS, GY), bf16),
            half, longer, half, longer,
            half, longer, half, longer, half, half,
            pltpu.VMEM((2 * ROWS, 2 * ROWS), F32),
            pltpu.VMEM((2 * ROWS, 2 * ROWS), F32),
            pltpu.VMEM((ROWS, ROWS), F32),
            pltpu.VMEM((ROWS, 128), F32),
            pltpu.VMEM((ROWS, 128), F32),
            pltpu.VMEM((ROWS, 128), F32),
            pltpu.VMEM((ROWS, 128), F32),
            pltpu.VMEM((8, 128), F32),
            pltpu.VMEM((8, 128), F32),
            pltpu.VMEM((8, 128), F32),
            pltpu.SemaphoreType.DMA((GX // TILE,)),
            pltpu.SemaphoreType.DMA((4, NCHUNK)),
            pltpu.SemaphoreType.DMA((4, NCHUNK)),
            pltpu.SemaphoreType.DMA((2, 2)),
            pltpu.SemaphoreType.DMA((2, 2)),
            pltpu.SemaphoreType.DMA((2, 2)),
        ],
        compiler_params=pltpu.CompilerParams(
            collective_id=0, has_side_effects=True, vmem_limit_bytes=56 << 20
        ),
    )(bands, umklapp, coeffs[0, 0])
    return flux, jnp.swapaxes(links, 2, 3)


def solution(mesh):
    in_specs = (P("kx", "ky", None, None, None, None), P(), P())
    out_specs = (P("kx", "ky", None), P("kx", "ky", None, None))
    return jax.shard_map(
        per_device, mesh=mesh, in_specs=in_specs, out_specs=out_specs, check_vma=False
    )
```

```python
import functools

import jax
import jax.numpy as jnp
from jax import lax
from jax.experimental import pallas as pl
from jax.experimental.pallas import tpu as pltpu
from jax.sharding import PartitionSpec as P

MESH = pl.DeviceIdType.MESH
NB = 32
ROWS = 2 * NB
GX = 128
GY = 256
HALF = GX // 2
EXTRA = 3
CHUNK = 8
NCHUNK = HALF // CHUNK
TILE = 16
GROUP = 8
RELAYED = (1, 1, 4, 4)
F32 = jnp.float32
CONTRACT = (((1,), (1,)), ((), ()))


def dot(a, b):
    return lax.dot_general(a, b, CONTRACT, preferred_element_type=F32)


def complex_parts(square):
    real = square[:NB, :NB] + square[NB:, NB:]
    imag = square[:NB, NB:] - square[NB:, :NB]
    return real, imag


def times(a, b):
    return a[0] * b[0] - a[1] * b[1], a[0] * b[1] + a[1] * b[0]


def conjugate(a):
    return a[0], -a[1]


def eliminate(wr, wi):
    lane = lax.broadcasted_iota(jnp.int32, (NB, 128), 1)
    row_id = lax.broadcasted_iota(jnp.int32, (NB, 128), 0)
    base = (lane // NB) * NB
    pivots_r, pivots_i = [], []
    for k in range(NB):
        where = base + k
        col_r = jnp.take_along_axis(wr, where, axis=1)
        col_i = jnp.take_along_axis(wi, where, axis=1)
        pr = col_r[k : k + 1]
        pi = col_i[k : k + 1]
        pivots_r.append(pr)
        pivots_i.append(pi)
        if k == NB - 1:
            break
        mag = pr * pr + pi * pi
        inv_r = pr / mag
        inv_i = -pi / mag
        below = row_id > k
        fr = jnp.where(below, col_r * inv_r - col_i * inv_i, 0.0)
        fi = jnp.where(below, col_r * inv_i + col_i * inv_r, 0.0)
        row_r = wr[k : k + 1]
        row_i = wi[k : k + 1]
        wr, wi = (
            wr - (fr * row_r - fi * row_i),
            wi - (fr * row_i + fi * row_r),
        )
    pr = jnp.concatenate(pivots_r, axis=0)
    pi = jnp.concatenate(pivots_i, axis=0)
    mag = jnp.sqrt(pr * pr + pi * pi)
    ur = pr / mag
    ui = pi / mag
    n = NB
    while n > 1:
        n //= 2
        ar, ai, br, bi = ur[:n], ui[:n], ur[n:], ui[n:]
        ur, ui = ar * br - ai * bi, ar * bi + ai * br
    return ur, ui


def kernel(
    bands, umk, coeffs, flux, links,
    cv, perm, u, zm, zp, xp, xm, szm, szp, sxp, sxm, wb, xb,
    acc_a, acc_b, acc_d, left_src, left_dst, down_src, down_dst,
    unit, unit_x, unit_y,
    hop, load_sem, send_sem, recv_sem, ez_sem, part_sem, unit_sem, hop_sem,
):
    i = lax.axis_index("kx")
    j = lax.axis_index("ky")
    ni = lax.axis_size("kx")
    nj = lax.axis_size("ky")
    right = (lax.rem(i + 1, ni), j)
    left = (lax.rem(i + ni - 1, ni), j)
    up = (i, lax.rem(j + 1, nj))
    down = (i, lax.rem(j + nj - 1, nj))
    x_edge = i == ni - 1
    y_edge = j == 0
    edge = jnp.logical_or(x_edge, y_edge)

    def load(t):
        rows = pl.ds(t * TILE, TILE)
        return pltpu.make_async_copy(coeffs.at[:, :, rows, :], cv[t], load_sem.at[t])

    half_tiles = HALF // TILE
    for t in range(half_tiles):
        load(t).start()
        load(t + half_tiles).start()

    def shifted(di, dj):
        return lax.rem(i + di + ni, ni), lax.rem(j + dj + nj, nj)

    in_row = lax.rem(i, GROUP)
    in_column = lax.rem(j, GROUP)
    first_plane = in_column == 0
    last_plane = in_column == GROUP - 1
    wrap_plane = jnp.logical_or(first_plane, last_plane)
    sends_by = (
        first_plane,
        last_plane,
        jnp.logical_and(wrap_plane, in_row == GROUP - 1),
        jnp.logical_and(wrap_plane, in_row == 0),
    )
    relay_of = (shifted(0, -2), shifted(0, 2), shifted(6, 0), shifted(-6, 0))
    is_relay = (
        in_column == GROUP - 2,
        in_column == 1,
        jnp.logical_and(wrap_plane, in_row == 5),
        jnp.logical_and(wrap_plane, in_row == 2),
    )
    relay_from = (shifted(0, 2), shifted(0, -2), shifted(-6, 0), shifted(6, 0))
    relay_to = (up, down, shifted(-5, 0), shifted(5, 0))
    gets_by = (None, None, sends_by[3], sends_by[2])
    gets_from = (None, None, shifted(5, 0), shifted(-5, 0))

    barrier = pltpu.get_barrier_semaphore()
    for device in (right, left, up, down):
        pl.semaphore_signal(barrier, inc=1, device_id=device, device_id_type=MESH)
    arrivals = jnp.int32(4)
    for flags, devices in (
        (sends_by, relay_of),
        (is_relay, relay_from),
        ((None, None, *is_relay[2:]), relay_to),
        (gets_by, gets_from),
    ):
        for flag, device in zip(flags, devices, strict=True):
            if flag is None:
                continue
            arrivals = arrivals + jnp.where(flag, 1, 0)

            @pl.when(flag)
            def _(device=device):
                pl.semaphore_signal(barrier, inc=1, device_id=device, device_id_type=MESH)

    zero = jnp.int32(0)
    ax = jnp.where(x_edge, umk[0, 0], zero)
    bx = jnp.where(x_edge, umk[0, 1], zero)
    ay = jnp.where(y_edge, umk[1, 0], zero)
    by = jnp.where(y_edge, umk[1, 1], zero)

    size = TILE * TILE
    to = lax.broadcasted_iota(jnp.int32, (size, size), 0)
    take = lax.broadcasted_iota(jnp.int32, (size, size), 1)
    swap = (to % TILE) * TILE + to // TILE
    perm[...] = jnp.where(take == swap, 1.0, 0.0).astype(jnp.bfloat16)

    acc_a[...] = jnp.zeros_like(acc_a)
    acc_b[...] = jnp.zeros_like(acc_b)
    acc_d[...] = jnp.zeros_like(acc_d)

    def remote(src, dst, stream, c, device):
        return pltpu.make_async_remote_copy(
            src_ref=src, dst_ref=dst, send_sem=send_sem.at[stream, c],
            recv_sem=recv_sem.at[stream, c], device_id=device, device_id_type=MESH,
        )

    def stream_ends(stream, c, special):
        low = pl.ds(c * CHUNK, CHUNK)
        high = pl.ds(HALF + c * CHUNK, CHUNK)
        own, src, dst, device = (
            (low, szm, zm, down),
            (high, szp, zp, up),
            (low, sxp, xp, right),
            (high, sxm, xm, left),
        )[stream]
        source = src.at[low] if special else u.at[own]
        return source, dst.at[low], device

    def stream_wait(stream, c):
        return remote(*stream_ends(stream, c, False)[:2], stream, c, right)

    def stream_send(stream, c, special, when):
        source, target, device = stream_ends(stream, c, special)
        if c >= RELAYED[stream]:

            @pl.when(when)
            def _():
                remote(source, target, stream, c, device).start()

            return

        @pl.when(jnp.logical_and(when, jnp.logical_not(sends_by[stream])))
        def _():
            remote(source, target, stream, c, device).start()

        @pl.when(jnp.logical_and(when, sends_by[stream]))
        def _():
            pltpu.make_async_remote_copy(
                src_ref=source, dst_ref=hop.at[pl.ds(c * CHUNK, CHUNK)],
                send_sem=send_sem.at[stream, c], recv_sem=hop_sem.at[0, c],
                device_id=relay_of[stream], device_id_type=MESH,
            ).start()

    def relay_copy(stream, c):
        source = hop.at[pl.ds(c * CHUNK, CHUNK)]
        target = stream_ends(stream, c, False)[1]
        return pltpu.make_async_remote_copy(
            src_ref=source, dst_ref=target, send_sem=hop_sem.at[1, c],
            recv_sem=recv_sem.at[stream, c], device_id=relay_to[stream],
            device_id_type=MESH,
        )

    def relay_arrival(c):
        rows = hop.at[pl.ds(c * CHUNK, CHUNK)]
        return pltpu.make_async_remote_copy(
            src_ref=rows, dst_ref=rows, send_sem=hop_sem.at[1, c],
            recv_sem=hop_sem.at[0, c], device_id=right, device_id_type=MESH,
        )

    need = (y_edge, x_edge, x_edge, y_edge)

    def gather(t):
        rows = pl.ds(t * TILE, TILE)
        for g in range(ROWS // TILE):
            r, b = divmod(g * TILE, NB)
            parts = [cv[t][r, bands[b + e]] for e in range(TILE)]
            moved = jnp.dot(perm[...], jnp.concatenate(parts, axis=0), preferred_element_type=F32)
            moved = moved.astype(jnp.bfloat16).reshape(TILE, TILE, GY)
            u[rows, pl.ds(g * TILE, TILE), :] = moved

    for t in range(half_tiles):
        load(t).wait()
        gather(t)
        load(t + half_tiles).wait()
        gather(t + half_tiles)
        if t == 0:
            pl.semaphore_wait(barrier, arrivals)
        for c in range(t * TILE // CHUNK, (t + 1) * TILE // CHUNK):
            for stream in range(4):
                stream_send(stream, c, False, jnp.logical_not(need[stream]))

    def build(dst, count, first, dp, dq):
        shift = lax.rem(GY - dq, GY)

        @pl.loop(0, count // 8)
        def _(c):
            for q in range(8):
                p = c * 8 + q
                row = lax.rem(first + p + dp + GX, GX)
                dst[p] = pltpu.roll(u[row], shift, 1)

    def build_extra(dst, forward, dq):
        shift = lax.rem(GY - dq, GY)
        for e in range(EXTRA):
            row = jnp.where(forward, e, HALF - EXTRA + e)
            dst[HALF + e] = pltpu.roll(u[row], shift, 1)

    def extra(stream, src, dst, device):
        rows = pl.ds(HALF, EXTRA)
        return pltpu.make_async_remote_copy(
            src_ref=src.at[rows], dst_ref=dst.at[rows], send_sem=ez_sem.at[0, stream],
            recv_sem=ez_sem.at[1, stream], device_id=device, device_id_type=MESH,
        )

    @pl.when(y_edge)
    def _():
        build(szm, HALF, 0, -ay, -by)
        for c in range(NCHUNK):
            stream_send(0, c, True, True)

    @pl.when(x_edge)
    def _():
        build(szp, HALF, HALF, 0, bx)
        build_extra(szp, ax > 0, bx)
        extra(0, szp, zp, up).start()
        for c in range(NCHUNK):
            stream_send(1, c, True, True)
        build(sxp, HALF, 0, ax, bx)
        for c in range(NCHUNK):
            stream_send(2, c, True, True)

    @pl.when(y_edge)
    def _():
        build(sxm, HALF, HALF, 0, -by)
        build_extra(sxm, ay < 0, -by)
        extra(1, sxm, xm, left).start()
        for c in range(NCHUNK):
            stream_send(3, c, True, True)

    for stream in range(4):

        @pl.when(is_relay[stream])
        def _(stream=stream):
            for c in range(RELAYED[stream]):
                relay_arrival(c).wait_recv()
                relay_copy(stream, c).start()

    build(wb, HALF, HALF, -ay, bx - by)
    build(xb, HALF, HALF, ax, bx - by)

    @pl.loop(0, NCHUNK)
    def _(c):
        for stream in range(4):
            stream_wait(stream, c).wait_recv()
        first = c * CHUNK
        a = None
        b = None
        for q in range(CHUNK):
            p = first + q
            own = u[p]
            lhs = jnp.concatenate([own, xp[p]], axis=0)
            rhs = jnp.concatenate([zm[p], own], axis=0)
            term = dot(lhs, rhs)
            a = term if a is None else a + term
            lhs = jnp.concatenate([zp[p], xb[p]], axis=0)
            rhs = jnp.concatenate([wb[p], xm[p]], axis=0)
            term = dot(lhs, rhs)
            b = term if b is None else b + term
        acc_a[...] += a
        acc_b[...] += b

    acc_d[...] = acc_b[:ROWS, ROWS:]

    @pl.when(x_edge)
    def _():
        extra(0, szp, zp, up).wait_recv()

    @pl.when(y_edge)
    def _():
        extra(1, sxm, xm, left).wait_recv()

    @pl.when(edge)
    def _():
        acc_d[...] = jnp.zeros_like(acc_d)

        @pl.loop(0, HALF // 8)
        def _(c):
            total = None
            for q in range(8):
                s = c * 8 + q + ax
                t = c * 8 + q - ay
                s = jnp.where(s < 0, s + HALF + EXTRA, s)
                t = jnp.where(t < 0, t + HALF + EXTRA, t)
                term = dot(zp[s], xm[t])
                total = term if total is None else total + term
            acc_d[...] += total

    a = acc_a[...]
    b = acc_b[...]
    d_low = complex_parts(a[ROWS:, :ROWS])
    x_low = complex_parts(a[ROWS:, ROWS:])
    y_low = complex_parts(a[:ROWS, :ROWS])
    y_high = complex_parts(b[:ROWS, :ROWS])
    x_high = complex_parts(b[ROWS:, ROWS:])
    d_high = complex_parts(acc_d[...])
    none = jnp.zeros((NB, NB), F32)

    for part in range(2):
        rows = pl.ds(part * NB, NB)
        left_src[rows, :] = jnp.concatenate([x_low[part], none, d_low[part], none], axis=1)
        down_src[rows, :] = jnp.concatenate([none, y_high[part], d_high[part], none], axis=1)

    def part_copy(which):
        src, dst, device = ((left_src, left_dst, left), (down_src, down_dst, down))[which]
        return pltpu.make_async_remote_copy(
            src_ref=src, dst_ref=dst, send_sem=part_sem.at[0, which],
            recv_sem=part_sem.at[1, which], device_id=device, device_id_type=MESH,
        )

    for which in range(2):
        part_copy(which).start()
    own = [
        jnp.concatenate([x_high[part], y_low[part], none, none], axis=1) for part in range(2)
    ]
    for which in range(2):
        part_copy(which).wait_recv()
    wr, wi = (
        own[part] + left_dst[pl.ds(part * NB, NB), :] + down_dst[pl.ds(part * NB, NB), :]
        for part in range(2)
    )
    lane = lax.broadcasted_iota(jnp.int32, (NB, 128), 1)
    unused = lane >= 3 * NB
    wr = jnp.where(unused, 1.0, wr)
    ur, ui = eliminate(wr, wi)
    unit[0:1, :] = ur
    unit[1:2, :] = ui

    def unit_copy(which):
        dst, device = ((unit_x, left), (unit_y, down))[which]
        return pltpu.make_async_remote_copy(
            src_ref=unit, dst_ref=dst, send_sem=unit_sem.at[0, which],
            recv_sem=unit_sem.at[1, which], device_id=device, device_id_type=MESH,
        )

    for which in range(2):
        unit_copy(which).start()
    for which in range(2):
        unit_copy(which).wait_recv()

    def group(ref, which):
        real, imag = ref[0:1, :], ref[1:2, :]
        if which:
            shift = 128 - which * NB
            real, imag = pltpu.roll(real, shift, 1), pltpu.roll(imag, shift, 1)
        return real, imag

    along_x, along_y, along_d = (group(unit, which) for which in range(3))
    y_next = group(unit_x, 1)
    x_next = group(unit_y, 0)
    first = times(times(along_x, y_next), conjugate(along_d))
    second = times(times(along_d, conjugate(x_next)), conjugate(along_y))
    is_real = lax.broadcasted_iota(jnp.int32, (1, 128), 1) == 0
    angle = jnp.arctan2(
        jnp.where(is_real, first[1], second[1]), jnp.where(is_real, first[0], second[0])
    )
    flux[0] = angle[:, :2]
    lane = lax.broadcasted_iota(jnp.int32, (1, 128), 1)
    for part in range(2):
        row = jnp.where(lane == 0, along_x[part], along_y[part])
        row = jnp.where(lane == 2, along_d[part], row)
        links[0, 0, part : part + 1, :] = row[:, :3]

    @pl.loop(0, NCHUNK)
    def _(c):
        for stream in range(4):
            stream_wait(stream, c).wait_send()

    @pl.when(x_edge)
    def _():
        extra(0, szp, zp, up).wait_send()

    @pl.when(y_edge)
    def _():
        extra(1, sxm, xm, left).wait_send()

    for stream in range(4):

        @pl.when(is_relay[stream])
        def _(stream=stream):
            for c in range(RELAYED[stream]):
                relay_copy(stream, c).wait_send()

    for which in range(2):
        part_copy(which).wait_send()
        unit_copy(which).wait_send()


def per_device(coeffs, bands, umklapp):
    bf16 = jnp.bfloat16
    half = pltpu.VMEM((HALF, ROWS, GY), bf16)
    longer = pltpu.VMEM((HALF + EXTRA, ROWS, GY), bf16)
    flux, links = pl.pallas_call(
        kernel,
        out_shape=(
            jax.ShapeDtypeStruct((1, 1, 2), F32),
            jax.ShapeDtypeStruct((1, 1, 2, 3), F32),
        ),
        in_specs=[
            pl.BlockSpec(memory_space=pltpu.SMEM),
            pl.BlockSpec(memory_space=pltpu.SMEM),
            pl.BlockSpec(memory_space=pl.ANY),
        ],
        out_specs=(pl.BlockSpec(memory_space=pltpu.VMEM),) * 2,
        scratch_shapes=[
            [pltpu.VMEM((*coeffs.shape[2:4], TILE, GY), bf16)] * (GX // TILE),
            pltpu.VMEM((TILE * TILE, TILE * TILE), bf16),
            pltpu.VMEM((GX, ROWS, GY), bf16),
            half, longer, half, longer,
            half, longer, half, longer, half, half,
            pltpu.VMEM((2 * ROWS, 2 * ROWS), F32),
            pltpu.VMEM((2 * ROWS, 2 * ROWS), F32),
            pltpu.VMEM((ROWS, ROWS), F32),
            pltpu.VMEM((ROWS, 128), F32),
            pltpu.VMEM((ROWS, 128), F32),
            pltpu.VMEM((ROWS, 128), F32),
            pltpu.VMEM((ROWS, 128), F32),
            pltpu.VMEM((8, 128), F32),
            pltpu.VMEM((8, 128), F32),
            pltpu.VMEM((8, 128), F32),
            pltpu.VMEM((max(RELAYED) * CHUNK, ROWS, GY), bf16),
            pltpu.SemaphoreType.DMA((GX // TILE,)),
            pltpu.SemaphoreType.DMA((4, NCHUNK)),
            pltpu.SemaphoreType.DMA((4, NCHUNK)),
            pltpu.SemaphoreType.DMA((2, 2)),
            pltpu.SemaphoreType.DMA((2, 2)),
            pltpu.SemaphoreType.DMA((2, 2)),
            pltpu.SemaphoreType.DMA((2, max(RELAYED))),
        ],
        compiler_params=pltpu.CompilerParams(
            collective_id=0, has_side_effects=True, vmem_limit_bytes=56 << 20
        ),
    )(bands, umklapp, coeffs[0, 0])
    return flux, jnp.swapaxes(links, 2, 3)


def solution(mesh):
    in_specs = (P("kx", "ky", None, None, None, None), P(), P())
    out_specs = (P("kx", "ky", None), P("kx", "ky", None, None))
    return jax.shard_map(
        per_device, mesh=mesh, in_specs=in_specs, out_specs=out_specs, check_vma=False
    )
```

```python
import functools

import jax
import jax.numpy as jnp
from jax import lax
from jax.experimental import pallas as pl
from jax.experimental.pallas import tpu as pltpu
from jax.sharding import PartitionSpec as P

MESH = pl.DeviceIdType.MESH
NB = 32
ROWS = 2 * NB
GX = 128
GY = 256
HALF = GX // 2
EXTRA = 3
CHUNK = 8
NCHUNK = HALF // CHUNK
TILE = 16
GROUP = 8
RELAYED = ((1,), (1,), (4, 5, 6, 7), (4, 5, 6, 7))
LATE = 4
F32 = jnp.float32
CONTRACT = (((1,), (1,)), ((), ()))


def dot(a, b):
    return lax.dot_general(a, b, CONTRACT, preferred_element_type=F32)


def complex_parts(square):
    real = square[:NB, :NB] + square[NB:, NB:]
    imag = square[:NB, NB:] - square[NB:, :NB]
    return real, imag


def times(a, b):
    return a[0] * b[0] - a[1] * b[1], a[0] * b[1] + a[1] * b[0]


def conjugate(a):
    return a[0], -a[1]


def eliminate(wr, wi):
    lane = lax.broadcasted_iota(jnp.int32, (NB, 128), 1)
    row_id = lax.broadcasted_iota(jnp.int32, (NB, 128), 0)
    base = (lane // NB) * NB
    pivots_r, pivots_i = [], []
    for k in range(NB):
        where = base + k
        col_r = jnp.take_along_axis(wr, where, axis=1)
        col_i = jnp.take_along_axis(wi, where, axis=1)
        pr = col_r[k : k + 1]
        pi = col_i[k : k + 1]
        pivots_r.append(pr)
        pivots_i.append(pi)
        if k == NB - 1:
            break
        mag = pr * pr + pi * pi
        inv_r = pr / mag
        inv_i = -pi / mag
        below = row_id > k
        fr = jnp.where(below, col_r * inv_r - col_i * inv_i, 0.0)
        fi = jnp.where(below, col_r * inv_i + col_i * inv_r, 0.0)
        row_r = wr[k : k + 1]
        row_i = wi[k : k + 1]
        wr, wi = (
            wr - (fr * row_r - fi * row_i),
            wi - (fr * row_i + fi * row_r),
        )
    pr = jnp.concatenate(pivots_r, axis=0)
    pi = jnp.concatenate(pivots_i, axis=0)
    mag = jnp.sqrt(pr * pr + pi * pi)
    ur = pr / mag
    ui = pi / mag
    n = NB
    while n > 1:
        n //= 2
        ar, ai, br, bi = ur[:n], ui[:n], ur[n:], ui[n:]
        ur, ui = ar * br - ai * bi, ar * bi + ai * br
    return ur, ui


def kernel(
    bands, umk, coeffs, flux, links,
    cv, perm, u, zm, zp, xp, xm, szm, szp, sxp, sxm, wb, xb,
    acc_a, acc_b, acc_d, left_src, left_dst, down_src, down_dst,
    unit, unit_x, unit_y,
    hop, load_sem, send_sem, recv_sem, ez_sem, part_sem, unit_sem, hop_sem,
):
    i = lax.axis_index("kx")
    j = lax.axis_index("ky")
    ni = lax.axis_size("kx")
    nj = lax.axis_size("ky")
    right = (lax.rem(i + 1, ni), j)
    left = (lax.rem(i + ni - 1, ni), j)
    up = (i, lax.rem(j + 1, nj))
    down = (i, lax.rem(j + nj - 1, nj))
    x_edge = i == ni - 1
    y_edge = j == 0
    edge = jnp.logical_or(x_edge, y_edge)

    def load(t):
        rows = pl.ds(t * TILE, TILE)
        return pltpu.make_async_copy(coeffs.at[:, :, rows, :], cv[t], load_sem.at[t])

    half_tiles = HALF // TILE
    load(0).start()
    load(half_tiles).start()

    def shifted(di, dj):
        return lax.rem(i + di + ni, ni), lax.rem(j + dj + nj, nj)

    in_row = lax.rem(i, GROUP)
    in_column = lax.rem(j, GROUP)
    first_plane = in_column == 0
    last_plane = in_column == GROUP - 1
    wrap_plane = jnp.logical_or(first_plane, last_plane)
    sends_by = (
        first_plane,
        last_plane,
        jnp.logical_and(wrap_plane, in_row == GROUP - 1),
        jnp.logical_and(wrap_plane, in_row == 0),
    )
    relay_of = (shifted(0, -2), shifted(0, 2), shifted(5, 0), shifted(-5, 0))
    is_relay = (
        in_column == GROUP - 2,
        in_column == 1,
        jnp.logical_and(wrap_plane, in_row == 4),
        jnp.logical_and(wrap_plane, in_row == 3),
    )
    relay_from = (shifted(0, 2), shifted(0, -2), shifted(-5, 0), shifted(5, 0))
    relay_to = (up, down, shifted(-4, 0), shifted(4, 0))
    gets_by = (None, None, sends_by[3], sends_by[2])
    gets_from = (None, None, shifted(4, 0), shifted(-4, 0))

    barrier = pltpu.get_barrier_semaphore()
    for device in (right, left, up, down):
        pl.semaphore_signal(barrier, inc=1, device_id=device, device_id_type=MESH)
    arrivals = jnp.int32(4)
    for flags, devices in (
        (sends_by, relay_of),
        (is_relay, relay_from),
        ((None, None, *is_relay[2:]), relay_to),
        (gets_by, gets_from),
    ):
        for flag, device in zip(flags, devices, strict=True):
            if flag is None:
                continue
            arrivals = arrivals + jnp.where(flag, 1, 0)

            @pl.when(flag)
            def _(device=device):
                pl.semaphore_signal(barrier, inc=1, device_id=device, device_id_type=MESH)

    zero = jnp.int32(0)
    ax = jnp.where(x_edge, umk[0, 0], zero)
    bx = jnp.where(x_edge, umk[0, 1], zero)
    ay = jnp.where(y_edge, umk[1, 0], zero)
    by = jnp.where(y_edge, umk[1, 1], zero)

    size = TILE * TILE
    to = lax.broadcasted_iota(jnp.int32, (size, size), 0)
    take = lax.broadcasted_iota(jnp.int32, (size, size), 1)
    swap = (to % TILE) * TILE + to // TILE
    perm[...] = jnp.where(take == swap, 1.0, 0.0).astype(jnp.bfloat16)

    acc_a[...] = jnp.zeros_like(acc_a)
    acc_b[...] = jnp.zeros_like(acc_b)
    acc_d[...] = jnp.zeros_like(acc_d)

    for t in range(1, half_tiles):
        load(t).start()
        load(t + half_tiles).start()

    def remote(src, dst, stream, c, device):
        return pltpu.make_async_remote_copy(
            src_ref=src, dst_ref=dst, send_sem=send_sem.at[stream, c],
            recv_sem=recv_sem.at[stream, c], device_id=device, device_id_type=MESH,
        )

    def stream_ends(stream, c, special):
        low = pl.ds(c * CHUNK, CHUNK)
        high = pl.ds(HALF + c * CHUNK, CHUNK)
        own, src, dst, device = (
            (low, szm, zm, down),
            (high, szp, zp, up),
            (low, sxp, xp, right),
            (high, sxm, xm, left),
        )[stream]
        source = src.at[low] if special else u.at[own]
        return source, dst.at[low], device

    def slot(stream, c):
        return pl.ds(RELAYED[stream].index(c) * CHUNK, CHUNK)

    def stream_wait(stream, c):
        return remote(*stream_ends(stream, c, False)[:2], stream, c, right)

    def stream_send(stream, c, special, when, first=False):
        source, target, device = stream_ends(stream, c, special)
        if first and stream < 2 and c >= LATE:
            when = jnp.logical_and(when, jnp.logical_not(is_relay[1 - stream]))
        if c not in RELAYED[stream]:

            @pl.when(when)
            def _():
                remote(source, target, stream, c, device).start()

            return

        @pl.when(jnp.logical_and(when, jnp.logical_not(sends_by[stream])))
        def _():
            remote(source, target, stream, c, device).start()

        @pl.when(jnp.logical_and(when, sends_by[stream]))
        def _():
            pltpu.make_async_remote_copy(
                src_ref=source, dst_ref=hop.at[slot(stream, c)],
                send_sem=send_sem.at[stream, c], recv_sem=hop_sem.at[0, c],
                device_id=relay_of[stream], device_id_type=MESH,
            ).start()

    def relay_copy(stream, c):
        source = hop.at[slot(stream, c)]
        target = stream_ends(stream, c, False)[1]
        return pltpu.make_async_remote_copy(
            src_ref=source, dst_ref=target, send_sem=hop_sem.at[1, c],
            recv_sem=recv_sem.at[stream, c], device_id=relay_to[stream],
            device_id_type=MESH,
        )

    def relay_arrival(stream, c):
        rows = hop.at[slot(stream, c)]
        return pltpu.make_async_remote_copy(
            src_ref=rows, dst_ref=rows, send_sem=hop_sem.at[1, c],
            recv_sem=hop_sem.at[0, c], device_id=right, device_id_type=MESH,
        )

    need = (y_edge, x_edge, x_edge, y_edge)

    def gather(t):
        rows = pl.ds(t * TILE, TILE)
        for g in range(ROWS // TILE):
            r, b = divmod(g * TILE, NB)
            parts = [cv[t][r, bands[b + e]] for e in range(TILE)]
            moved = jnp.dot(perm[...], jnp.concatenate(parts, axis=0), preferred_element_type=F32)
            moved = moved.astype(jnp.bfloat16).reshape(TILE, TILE, GY)
            u[rows, pl.ds(g * TILE, TILE), :] = moved

    for t in range(half_tiles):
        load(t).wait()
        gather(t)
        load(t + half_tiles).wait()
        gather(t + half_tiles)
        if t == 0:
            pl.semaphore_wait(barrier, arrivals)
        for c in range(t * TILE // CHUNK, (t + 1) * TILE // CHUNK):
            for stream in range(4):
                stream_send(stream, c, False, jnp.logical_not(need[stream]), True)

    def build(dst, count, first, dp, dq):
        shift = lax.rem(GY - dq, GY)

        @pl.loop(0, count // 8)
        def _(c):
            for q in range(8):
                p = c * 8 + q
                row = lax.rem(first + p + dp + GX, GX)
                dst[p] = pltpu.roll(u[row], shift, 1)

    def build_extra(dst, forward, dq):
        shift = lax.rem(GY - dq, GY)
        for e in range(EXTRA):
            row = jnp.where(forward, e, HALF - EXTRA + e)
            dst[HALF + e] = pltpu.roll(u[row], shift, 1)

    def extra(stream, src, dst, device):
        rows = pl.ds(HALF, EXTRA)
        return pltpu.make_async_remote_copy(
            src_ref=src.at[rows], dst_ref=dst.at[rows], send_sem=ez_sem.at[0, stream],
            recv_sem=ez_sem.at[1, stream], device_id=device, device_id_type=MESH,
        )

    @pl.when(y_edge)
    def _():
        build(szm, HALF, 0, -ay, -by)
        for c in range(NCHUNK):
            stream_send(0, c, True, True, True)

    @pl.when(x_edge)
    def _():
        build(szp, HALF, HALF, 0, bx)
        build_extra(szp, ax > 0, bx)
        extra(0, szp, zp, up).start()
        for c in range(NCHUNK):
            stream_send(1, c, True, True, True)
        build(sxp, HALF, 0, ax, bx)
        for c in range(NCHUNK):
            stream_send(2, c, True, True, True)

    @pl.when(y_edge)
    def _():
        build(sxm, HALF, HALF, 0, -by)
        build_extra(sxm, ay < 0, -by)
        extra(1, sxm, xm, left).start()
        for c in range(NCHUNK):
            stream_send(3, c, True, True, True)

    for stream in range(4):

        @pl.when(is_relay[stream])
        def _(stream=stream):
            for c in RELAYED[stream]:
                relay_arrival(stream, c).wait_recv()
                relay_copy(stream, c).start()
            if stream < 2:
                other = 1 - stream
                for c in range(LATE, NCHUNK):
                    stream_send(other, c, False, jnp.logical_not(need[other]))
                    stream_send(other, c, True, need[other])

    build(wb, HALF, HALF, -ay, bx - by)
    build(xb, HALF, HALF, ax, bx - by)

    @pl.loop(0, NCHUNK)
    def _(step):
        early, late = RELAYED[0][0], len(RELAYED[0])
        c = jnp.where(step < early, step, step + late)
        c = jnp.where(step < NCHUNK - late, c, early + step - (NCHUNK - late))
        for stream in range(4):
            stream_wait(stream, c).wait_recv()
        first = c * CHUNK
        a = None
        b = None
        for q in range(CHUNK):
            p = first + q
            own = u[p]
            lhs = jnp.concatenate([own, xp[p]], axis=0)
            rhs = jnp.concatenate([zm[p], own], axis=0)
            term = dot(lhs, rhs)
            a = term if a is None else a + term
            lhs = jnp.concatenate([zp[p], xb[p]], axis=0)
            rhs = jnp.concatenate([wb[p], xm[p]], axis=0)
            term = dot(lhs, rhs)
            b = term if b is None else b + term
        acc_a[...] += a
        acc_b[...] += b

    acc_d[...] = acc_b[:ROWS, ROWS:]

    @pl.when(x_edge)
    def _():
        extra(0, szp, zp, up).wait_recv()

    @pl.when(y_edge)
    def _():
        extra(1, sxm, xm, left).wait_recv()

    @pl.when(edge)
    def _():
        acc_d[...] = jnp.zeros_like(acc_d)

        @pl.loop(0, HALF // 32)
        def _(c):
            total = None
            for q in range(32):
                s = c * 32 + q + ax
                t = c * 32 + q - ay
                s = jnp.where(s < 0, s + HALF + EXTRA, s)
                t = jnp.where(t < 0, t + HALF + EXTRA, t)
                term = dot(zp[s], xm[t])
                total = term if total is None else total + term
            acc_d[...] += total

    a = acc_a[...]
    b = acc_b[...]
    d_low = complex_parts(a[ROWS:, :ROWS])
    x_low = complex_parts(a[ROWS:, ROWS:])
    y_low = complex_parts(a[:ROWS, :ROWS])
    y_high = complex_parts(b[:ROWS, :ROWS])
    x_high = complex_parts(b[ROWS:, ROWS:])
    d_high = complex_parts(acc_d[...])
    none = jnp.zeros((NB, NB), F32)

    for part in range(2):
        rows = pl.ds(part * NB, NB)
        left_src[rows, :] = jnp.concatenate([x_low[part], none, d_low[part], none], axis=1)
        down_src[rows, :] = jnp.concatenate([none, y_high[part], d_high[part], none], axis=1)

    def part_copy(which):
        src, dst, device = ((left_src, left_dst, left), (down_src, down_dst, down))[which]
        return pltpu.make_async_remote_copy(
            src_ref=src, dst_ref=dst, send_sem=part_sem.at[0, which],
            recv_sem=part_sem.at[1, which], device_id=device, device_id_type=MESH,
        )

    for which in range(2):
        part_copy(which).start()
    own = [
        jnp.concatenate([x_high[part], y_low[part], none, none], axis=1) for part in range(2)
    ]
    for which in range(2):
        part_copy(which).wait_recv()
    wr, wi = (
        own[part] + left_dst[pl.ds(part * NB, NB), :] + down_dst[pl.ds(part * NB, NB), :]
        for part in range(2)
    )
    lane = lax.broadcasted_iota(jnp.int32, (NB, 128), 1)
    unused = lane >= 3 * NB
    wr = jnp.where(unused, 1.0, wr)
    ur, ui = eliminate(wr, wi)
    unit[0:1, :] = ur
    unit[1:2, :] = ui

    def unit_copy(which):
        dst, device = ((unit_x, left), (unit_y, down))[which]
        return pltpu.make_async_remote_copy(
            src_ref=unit, dst_ref=dst, send_sem=unit_sem.at[0, which],
            recv_sem=unit_sem.at[1, which], device_id=device, device_id_type=MESH,
        )

    for which in range(2):
        unit_copy(which).start()
    for which in range(2):
        unit_copy(which).wait_recv()

    def group(ref, which):
        real, imag = ref[0:1, :], ref[1:2, :]
        if which:
            shift = 128 - which * NB
            real, imag = pltpu.roll(real, shift, 1), pltpu.roll(imag, shift, 1)
        return real, imag

    along_x, along_y, along_d = (group(unit, which) for which in range(3))
    y_next = group(unit_x, 1)
    x_next = group(unit_y, 0)
    first = times(times(along_x, y_next), conjugate(along_d))
    second = times(times(along_d, conjugate(x_next)), conjugate(along_y))
    is_real = lax.broadcasted_iota(jnp.int32, (1, 128), 1) == 0
    angle = jnp.arctan2(
        jnp.where(is_real, first[1], second[1]), jnp.where(is_real, first[0], second[0])
    )
    flux[0] = angle[:, :2]
    lane = lax.broadcasted_iota(jnp.int32, (1, 128), 1)
    for part in range(2):
        row = jnp.where(lane == 0, along_x[part], along_y[part])
        row = jnp.where(lane == 2, along_d[part], row)
        links[0, 0, part : part + 1, :] = row[:, :3]

    @pl.loop(0, NCHUNK)
    def _(c):
        for stream in range(4):
            stream_wait(stream, c).wait_send()

    @pl.when(x_edge)
    def _():
        extra(0, szp, zp, up).wait_send()

    @pl.when(y_edge)
    def _():
        extra(1, sxm, xm, left).wait_send()

    for stream in range(4):

        @pl.when(is_relay[stream])
        def _(stream=stream):
            for c in RELAYED[stream]:
                relay_copy(stream, c).wait_send()

    for which in range(2):
        part_copy(which).wait_send()
        unit_copy(which).wait_send()


def per_device(coeffs, bands, umklapp):
    bf16 = jnp.bfloat16
    half = pltpu.VMEM((HALF, ROWS, GY), bf16)
    longer = pltpu.VMEM((HALF + EXTRA, ROWS, GY), bf16)
    flux, links = pl.pallas_call(
        kernel,
        out_shape=(
            jax.ShapeDtypeStruct((1, 1, 2), F32),
            jax.ShapeDtypeStruct((1, 1, 2, 3), F32),
        ),
        in_specs=[
            pl.BlockSpec(memory_space=pltpu.SMEM),
            pl.BlockSpec(memory_space=pltpu.SMEM),
            pl.BlockSpec(memory_space=pl.ANY),
        ],
        out_specs=(pl.BlockSpec(memory_space=pltpu.VMEM),) * 2,
        scratch_shapes=[
            [pltpu.VMEM((*coeffs.shape[2:4], TILE, GY), bf16)] * (GX // TILE),
            pltpu.VMEM((TILE * TILE, TILE * TILE), bf16),
            pltpu.VMEM((GX, ROWS, GY), bf16),
            half, longer, half, longer,
            half, longer, half, longer, half, half,
            pltpu.VMEM((2 * ROWS, 2 * ROWS), F32),
            pltpu.VMEM((2 * ROWS, 2 * ROWS), F32),
            pltpu.VMEM((ROWS, ROWS), F32),
            pltpu.VMEM((ROWS, 128), F32),
            pltpu.VMEM((ROWS, 128), F32),
            pltpu.VMEM((ROWS, 128), F32),
            pltpu.VMEM((ROWS, 128), F32),
            pltpu.VMEM((8, 128), F32),
            pltpu.VMEM((8, 128), F32),
            pltpu.VMEM((8, 128), F32),
            pltpu.VMEM((max(map(len, RELAYED)) * CHUNK, ROWS, GY), bf16),
            pltpu.SemaphoreType.DMA((GX // TILE,)),
            pltpu.SemaphoreType.DMA((4, NCHUNK)),
            pltpu.SemaphoreType.DMA((4, NCHUNK)),
            pltpu.SemaphoreType.DMA((2, 2)),
            pltpu.SemaphoreType.DMA((2, 2)),
            pltpu.SemaphoreType.DMA((2, 2)),
            pltpu.SemaphoreType.DMA((2, NCHUNK)),
        ],
        compiler_params=pltpu.CompilerParams(
            collective_id=0, has_side_effects=True, vmem_limit_bytes=56 << 20
        ),
    )(bands, umklapp, coeffs[0, 0])
    return flux, jnp.swapaxes(links, 2, 3)


def solution(mesh):
    in_specs = (P("kx", "ky", None, None, None, None), P(), P())
    out_specs = (P("kx", "ky", None), P("kx", "ky", None, None))
    return jax.shard_map(
        per_device, mesh=mesh, in_specs=in_specs, out_specs=out_specs, check_vma=False
    )
```

```python
import functools

import jax
import jax.numpy as jnp
from jax import lax
from jax.experimental import pallas as pl
from jax.experimental.pallas import tpu as pltpu
from jax.sharding import PartitionSpec as P

MESH = pl.DeviceIdType.MESH
NB = 32
ROWS = 2 * NB
GX = 128
GY = 256
HALF = GX // 2
EXTRA = 3
CHUNK = 8
NCHUNK = HALF // CHUNK
TILE = 16
GROUP = 8
RELAYED = ((1,), (1,), (4, 5, 6, 7), (4, 5, 6, 7))
LATE = 4
F32 = jnp.float32
CONTRACT = (((1,), (1,)), ((), ()))


def dot(a, b):
    return lax.dot_general(a, b, CONTRACT, preferred_element_type=F32)


def complex_parts(square):
    real = square[:NB, :NB] + square[NB:, NB:]
    imag = square[:NB, NB:] - square[NB:, :NB]
    return real, imag


def times(a, b):
    return a[0] * b[0] - a[1] * b[1], a[0] * b[1] + a[1] * b[0]


def conjugate(a):
    return a[0], -a[1]


def eliminate(tiles):
    lane = lax.broadcasted_iota(jnp.int32, (NB, 128), 1)
    row_id = lax.broadcasted_iota(jnp.int32, (NB, 128), 0)
    base = (lane // NB) * NB
    tiles = list(tiles)
    pivots = [([], []) for _ in tiles]
    for k in range(NB):
        where = base + k
        below = row_id > k
        for n, (wr, wi) in enumerate(tiles):
            col_r = jnp.take_along_axis(wr, where, axis=1)
            col_i = jnp.take_along_axis(wi, where, axis=1)
            pr = col_r[k : k + 1]
            pi = col_i[k : k + 1]
            pivots[n][0].append(pr)
            pivots[n][1].append(pi)
            if k == NB - 1:
                continue
            mag = pr * pr + pi * pi
            inv_r = pr / mag
            inv_i = -pi / mag
            fr = jnp.where(below, col_r * inv_r - col_i * inv_i, 0.0)
            fi = jnp.where(below, col_r * inv_i + col_i * inv_r, 0.0)
            row_r = wr[k : k + 1]
            row_i = wi[k : k + 1]
            tiles[n] = (
                wr - (fr * row_r - fi * row_i),
                wi - (fr * row_i + fi * row_r),
            )
    return [unit_product(*(jnp.concatenate(part, axis=0) for part in p)) for p in pivots]


def unit_product(pr, pi):
    mag = jnp.sqrt(pr * pr + pi * pi)
    ur = pr / mag
    ui = pi / mag
    n = NB
    while n > 1:
        n //= 2
        ar, ai, br, bi = ur[:n], ui[:n], ur[n:], ui[n:]
        ur, ui = ar * br - ai * bi, ar * bi + ai * br
    return ur, ui


def kernel(
    bands, umk, coeffs, flux, links,
    cv, perm, u, zm, zp, xp, xm, szm, szp, sxp, sxm, wb, xb,
    acc_a, acc_b, acc_d, left_src, left_dst, down_src, down_dst, corner_src, corner_dst,
    hop, load_sem, send_sem, recv_sem, ez_sem, part_sem, hop_sem,
):
    i = lax.axis_index("kx")
    j = lax.axis_index("ky")
    ni = lax.axis_size("kx")
    nj = lax.axis_size("ky")
    right = (lax.rem(i + 1, ni), j)
    left = (lax.rem(i + ni - 1, ni), j)
    up = (i, lax.rem(j + 1, nj))
    down = (i, lax.rem(j + nj - 1, nj))
    x_edge = i == ni - 1
    y_edge = j == 0
    edge = jnp.logical_or(x_edge, y_edge)

    def load(t):
        rows = pl.ds(t * TILE, TILE)
        return pltpu.make_async_copy(coeffs.at[:, :, rows, :], cv[t], load_sem.at[t])

    half_tiles = HALF // TILE
    load(0).start()
    load(half_tiles).start()

    def shifted(di, dj):
        return lax.rem(i + di + ni, ni), lax.rem(j + dj + nj, nj)

    in_row = lax.rem(i, GROUP)
    in_column = lax.rem(j, GROUP)
    first_plane = in_column == 0
    last_plane = in_column == GROUP - 1
    wrap_plane = jnp.logical_or(first_plane, last_plane)
    sends_by = (
        first_plane,
        last_plane,
        jnp.logical_and(wrap_plane, in_row == GROUP - 1),
        jnp.logical_and(wrap_plane, in_row == 0),
    )
    relay_of = (shifted(0, -2), shifted(0, 2), shifted(5, 0), shifted(-5, 0))
    is_relay = (
        in_column == GROUP - 2,
        in_column == 1,
        jnp.logical_and(wrap_plane, in_row == 4),
        jnp.logical_and(wrap_plane, in_row == 3),
    )
    relay_from = (shifted(0, 2), shifted(0, -2), shifted(-5, 0), shifted(5, 0))
    relay_to = (up, down, shifted(-4, 0), shifted(4, 0))
    gets_by = (None, None, sends_by[3], sends_by[2])
    gets_from = (None, None, shifted(4, 0), shifted(-4, 0))

    barrier = pltpu.get_barrier_semaphore()
    for device in (right, left, up, down, shifted(1, 1), shifted(-1, -1)):
        pl.semaphore_signal(barrier, inc=1, device_id=device, device_id_type=MESH)
    arrivals = jnp.int32(6)
    for flags, devices in (
        (sends_by, relay_of),
        (is_relay, relay_from),
        ((None, None, *is_relay[2:]), relay_to),
        (gets_by, gets_from),
    ):
        for flag, device in zip(flags, devices, strict=True):
            if flag is None:
                continue
            arrivals = arrivals + jnp.where(flag, 1, 0)

            @pl.when(flag)
            def _(device=device):
                pl.semaphore_signal(barrier, inc=1, device_id=device, device_id_type=MESH)

    zero = jnp.int32(0)
    ax = jnp.where(x_edge, umk[0, 0], zero)
    bx = jnp.where(x_edge, umk[0, 1], zero)
    ay = jnp.where(y_edge, umk[1, 0], zero)
    by = jnp.where(y_edge, umk[1, 1], zero)

    size = TILE * TILE
    to = lax.broadcasted_iota(jnp.int32, (size, size), 0)
    take = lax.broadcasted_iota(jnp.int32, (size, size), 1)
    swap = (to % TILE) * TILE + to // TILE
    perm[...] = jnp.where(take == swap, 1.0, 0.0).astype(jnp.bfloat16)

    acc_a[...] = jnp.zeros_like(acc_a)
    acc_b[...] = jnp.zeros_like(acc_b)
    acc_d[...] = jnp.zeros_like(acc_d)

    for t in range(1, half_tiles):
        load(t).start()
        load(t + half_tiles).start()

    def remote(src, dst, stream, c, device):
        return pltpu.make_async_remote_copy(
            src_ref=src, dst_ref=dst, send_sem=send_sem.at[stream, c],
            recv_sem=recv_sem.at[stream, c], device_id=device, device_id_type=MESH,
        )

    def stream_ends(stream, c, special):
        low = pl.ds(c * CHUNK, CHUNK)
        high = pl.ds(HALF + c * CHUNK, CHUNK)
        own, src, dst, device = (
            (low, szm, zm, down),
            (high, szp, zp, up),
            (low, sxp, xp, right),
            (high, sxm, xm, left),
        )[stream]
        source = src.at[low] if special else u.at[own]
        return source, dst.at[low], device

    def slot(stream, c):
        return pl.ds(RELAYED[stream].index(c) * CHUNK, CHUNK)

    def stream_wait(stream, c):
        return remote(*stream_ends(stream, c, False)[:2], stream, c, right)

    def stream_send(stream, c, special, when, first=False):
        source, target, device = stream_ends(stream, c, special)
        if first and stream < 2 and c >= LATE:
            when = jnp.logical_and(when, jnp.logical_not(is_relay[1 - stream]))
        if c not in RELAYED[stream]:

            @pl.when(when)
            def _():
                remote(source, target, stream, c, device).start()

            return

        @pl.when(jnp.logical_and(when, jnp.logical_not(sends_by[stream])))
        def _():
            remote(source, target, stream, c, device).start()

        @pl.when(jnp.logical_and(when, sends_by[stream]))
        def _():
            pltpu.make_async_remote_copy(
                src_ref=source, dst_ref=hop.at[slot(stream, c)],
                send_sem=send_sem.at[stream, c], recv_sem=hop_sem.at[0, c],
                device_id=relay_of[stream], device_id_type=MESH,
            ).start()

    def relay_copy(stream, c):
        source = hop.at[slot(stream, c)]
        target = stream_ends(stream, c, False)[1]
        return pltpu.make_async_remote_copy(
            src_ref=source, dst_ref=target, send_sem=hop_sem.at[1, c],
            recv_sem=recv_sem.at[stream, c], device_id=relay_to[stream],
            device_id_type=MESH,
        )

    def relay_arrival(stream, c):
        rows = hop.at[slot(stream, c)]
        return pltpu.make_async_remote_copy(
            src_ref=rows, dst_ref=rows, send_sem=hop_sem.at[1, c],
            recv_sem=hop_sem.at[0, c], device_id=right, device_id_type=MESH,
        )

    need = (y_edge, x_edge, x_edge, y_edge)

    def gather(t):
        rows = pl.ds(t * TILE, TILE)
        for g in range(ROWS // TILE):
            r, b = divmod(g * TILE, NB)
            parts = [cv[t][r, bands[b + e]] for e in range(TILE)]
            moved = jnp.dot(perm[...], jnp.concatenate(parts, axis=0), preferred_element_type=F32)
            moved = moved.astype(jnp.bfloat16).reshape(TILE, TILE, GY)
            u[rows, pl.ds(g * TILE, TILE), :] = moved

    for t in range(half_tiles):
        load(t).wait()
        gather(t)
        load(t + half_tiles).wait()
        gather(t + half_tiles)
        if t == 0:
            pl.semaphore_wait(barrier, arrivals)
        for c in range(t * TILE // CHUNK, (t + 1) * TILE // CHUNK):
            for stream in range(4):
                stream_send(stream, c, False, jnp.logical_not(need[stream]), True)

    def build(dst, count, first, dp, dq):
        shift = lax.rem(GY - dq, GY)

        @pl.loop(0, count // 8)
        def _(c):
            for q in range(8):
                p = c * 8 + q
                row = lax.rem(first + p + dp + GX, GX)
                dst[p] = pltpu.roll(u[row], shift, 1)

    def build_extra(dst, forward, dq):
        shift = lax.rem(GY - dq, GY)
        for e in range(EXTRA):
            row = jnp.where(forward, e, HALF - EXTRA + e)
            dst[HALF + e] = pltpu.roll(u[row], shift, 1)

    def extra(stream, src, dst, device):
        rows = pl.ds(HALF, EXTRA)
        return pltpu.make_async_remote_copy(
            src_ref=src.at[rows], dst_ref=dst.at[rows], send_sem=ez_sem.at[0, stream],
            recv_sem=ez_sem.at[1, stream], device_id=device, device_id_type=MESH,
        )

    @pl.when(y_edge)
    def _():
        build(szm, HALF, 0, -ay, -by)
        for c in range(NCHUNK):
            stream_send(0, c, True, True, True)

    @pl.when(x_edge)
    def _():
        build(szp, HALF, HALF, 0, bx)
        build_extra(szp, ax > 0, bx)
        extra(0, szp, zp, up).start()
        for c in range(NCHUNK):
            stream_send(1, c, True, True, True)
        build(sxp, HALF, 0, ax, bx)
        for c in range(NCHUNK):
            stream_send(2, c, True, True, True)

    @pl.when(y_edge)
    def _():
        build(sxm, HALF, HALF, 0, -by)
        build_extra(sxm, ay < 0, -by)
        extra(1, sxm, xm, left).start()
        for c in range(NCHUNK):
            stream_send(3, c, True, True, True)

    for stream in range(4):

        @pl.when(is_relay[stream])
        def _(stream=stream):
            for c in RELAYED[stream]:
                relay_arrival(stream, c).wait_recv()
                relay_copy(stream, c).start()
            if stream < 2:
                other = 1 - stream
                for c in range(LATE, NCHUNK):
                    stream_send(other, c, False, jnp.logical_not(need[other]))
                    stream_send(other, c, True, need[other])

    build(wb, HALF, HALF, -ay, bx - by)
    build(xb, HALF, HALF, ax, bx - by)

    @pl.loop(0, NCHUNK)
    def _(step):
        early, late = RELAYED[0][0], len(RELAYED[0])
        c = jnp.where(step < early, step, step + late)
        c = jnp.where(step < NCHUNK - late, c, early + step - (NCHUNK - late))
        for stream in range(4):
            stream_wait(stream, c).wait_recv()
        first = c * CHUNK
        a = None
        b = None
        for q in range(CHUNK):
            p = first + q
            own = u[p]
            lhs = jnp.concatenate([own, xp[p]], axis=0)
            rhs = jnp.concatenate([zm[p], own], axis=0)
            term = dot(lhs, rhs)
            a = term if a is None else a + term
            lhs = jnp.concatenate([zp[p], xb[p]], axis=0)
            rhs = jnp.concatenate([wb[p], xm[p]], axis=0)
            term = dot(lhs, rhs)
            b = term if b is None else b + term
        acc_a[...] += a
        acc_b[...] += b

    acc_d[...] = acc_b[:ROWS, ROWS:]

    @pl.when(x_edge)
    def _():
        extra(0, szp, zp, up).wait_recv()

    @pl.when(y_edge)
    def _():
        extra(1, sxm, xm, left).wait_recv()

    @pl.when(edge)
    def _():
        acc_d[...] = jnp.zeros_like(acc_d)

        @pl.loop(0, HALF // 32)
        def _(c):
            total = None
            for q in range(32):
                s = c * 32 + q + ax
                t = c * 32 + q - ay
                s = jnp.where(s < 0, s + HALF + EXTRA, s)
                t = jnp.where(t < 0, t + HALF + EXTRA, t)
                term = dot(zp[s], xm[t])
                total = term if total is None else total + term
            acc_d[...] += total

    a = acc_a[...]
    b = acc_b[...]
    d_low = complex_parts(a[ROWS:, :ROWS])
    x_low = complex_parts(a[ROWS:, ROWS:])
    y_low = complex_parts(a[:ROWS, :ROWS])
    y_high = complex_parts(b[:ROWS, :ROWS])
    x_high = complex_parts(b[ROWS:, ROWS:])
    d_high = complex_parts(acc_d[...])
    none = jnp.zeros((NB, NB), F32)

    lane = lax.broadcasted_iota(jnp.int32, (NB, 128), 1)
    low, high = [], []
    for part in range(2):
        rows = pl.ds(part * NB, NB)
        low.append(jnp.concatenate([x_low[part], y_low[part], d_low[part], none], axis=1))
        high.append(jnp.concatenate([x_high[part], y_high[part], d_high[part], none], axis=1))
        left_src[rows, :] = low[part]
        down_src[rows, :] = high[part]
        corner_src[rows, :] = jnp.where(lane < NB, low[part], high[part])

    def part_copy(which):
        src, dst, device = (
            (left_src, left_dst, left),
            (down_src, down_dst, down),
            (corner_src, corner_dst, shifted(-1, -1)),
        )[which]
        return pltpu.make_async_remote_copy(
            src_ref=src, dst_ref=dst, send_sem=part_sem.at[0, which],
            recv_sem=part_sem.at[1, which], device_id=device, device_id_type=MESH,
        )

    for which in (2, 1, 0):
        part_copy(which).start()
    for which in range(3):
        part_copy(which).wait_recv()
    own_tile, next_tile = [], []
    for part in range(2):
        rows = pl.ds(part * NB, NB)
        of_left, of_down, of_corner = left_dst[rows, :], down_dst[rows, :], corner_dst[rows, :]
        other = jnp.where(lane < 2 * NB, low[part] + of_down, of_left + of_down)
        other = jnp.where(lane < NB, high[part] + of_left, other)
        own_tile.append(jnp.where(lane < 3 * NB, other, 1.0))
        other = of_corner + jnp.where(lane < NB, of_down, of_left)
        next_tile.append(jnp.where(lane < 2 * NB, other, 1.0))
    unit, unit_next = eliminate((own_tile, next_tile))

    def group(ref, which):
        real, imag = ref
        if which:
            shift = 128 - which * NB
            real, imag = pltpu.roll(real, shift, 1), pltpu.roll(imag, shift, 1)
        return real, imag

    along_x, along_y, along_d = (group(unit, which) for which in range(3))
    y_next = group(unit_next, 1)
    x_next = group(unit_next, 0)
    first = times(times(along_x, y_next), conjugate(along_d))
    second = times(times(along_d, conjugate(x_next)), conjugate(along_y))
    lane = lax.broadcasted_iota(jnp.int32, (1, 128), 1)
    angle = jnp.arctan2(
        jnp.where(lane == 0, first[1], second[1]), jnp.where(lane == 0, first[0], second[0])
    )
    flux[0] = angle[:, :2]
    for part in range(2):
        row = jnp.where(lane == 0, along_x[part], along_y[part])
        row = jnp.where(lane == 2, along_d[part], row)
        links[0, 0, part : part + 1, :] = row[:, :3]

    @pl.loop(0, NCHUNK)
    def _(c):
        for stream in range(4):
            stream_wait(stream, c).wait_send()

    @pl.when(x_edge)
    def _():
        extra(0, szp, zp, up).wait_send()

    @pl.when(y_edge)
    def _():
        extra(1, sxm, xm, left).wait_send()

    for stream in range(4):

        @pl.when(is_relay[stream])
        def _(stream=stream):
            for c in RELAYED[stream]:
                relay_copy(stream, c).wait_send()

    for which in range(3):
        part_copy(which).wait_send()


def per_device(coeffs, bands, umklapp):
    bf16 = jnp.bfloat16
    half = pltpu.VMEM((HALF, ROWS, GY), bf16)
    longer = pltpu.VMEM((HALF + EXTRA, ROWS, GY), bf16)
    flux, links = pl.pallas_call(
        kernel,
        out_shape=(
            jax.ShapeDtypeStruct((1, 1, 2), F32),
            jax.ShapeDtypeStruct((1, 1, 2, 3), F32),
        ),
        in_specs=[
            pl.BlockSpec(memory_space=pltpu.SMEM),
            pl.BlockSpec(memory_space=pltpu.SMEM),
            pl.BlockSpec(memory_space=pl.ANY),
        ],
        out_specs=(pl.BlockSpec(memory_space=pltpu.VMEM),) * 2,
        scratch_shapes=[
            [pltpu.VMEM((*coeffs.shape[2:4], TILE, GY), bf16)] * (GX // TILE),
            pltpu.VMEM((TILE * TILE, TILE * TILE), bf16),
            pltpu.VMEM((GX, ROWS, GY), bf16),
            half, longer, half, longer,
            half, longer, half, longer, half, half,
            pltpu.VMEM((2 * ROWS, 2 * ROWS), F32),
            pltpu.VMEM((2 * ROWS, 2 * ROWS), F32),
            pltpu.VMEM((ROWS, ROWS), F32),
            pltpu.VMEM((ROWS, 128), F32),
            pltpu.VMEM((ROWS, 128), F32),
            pltpu.VMEM((ROWS, 128), F32),
            pltpu.VMEM((ROWS, 128), F32),
            pltpu.VMEM((ROWS, 128), F32),
            pltpu.VMEM((ROWS, 128), F32),
            pltpu.VMEM((max(map(len, RELAYED)) * CHUNK, ROWS, GY), bf16),
            pltpu.SemaphoreType.DMA((GX // TILE,)),
            pltpu.SemaphoreType.DMA((4, NCHUNK)),
            pltpu.SemaphoreType.DMA((4, NCHUNK)),
            pltpu.SemaphoreType.DMA((2, 2)),
            pltpu.SemaphoreType.DMA((2, 3)),
            pltpu.SemaphoreType.DMA((2, NCHUNK)),
        ],
        compiler_params=pltpu.CompilerParams(
            collective_id=0, has_side_effects=True, vmem_limit_bytes=56 << 20
        ),
    )(bands, umklapp, coeffs[0, 0])
    return flux, jnp.swapaxes(links, 2, 3)


def solution(mesh):
    in_specs = (P("kx", "ky", None, None, None, None), P(), P())
    out_specs = (P("kx", "ky", None), P("kx", "ky", None, None))
    return jax.shard_map(
        per_device, mesh=mesh, in_specs=in_specs, out_specs=out_specs, check_vma=False
    )
```

```python
import functools

import jax
import jax.numpy as jnp
from jax import lax
from jax.experimental import pallas as pl
from jax.experimental.pallas import tpu as pltpu
from jax.sharding import PartitionSpec as P

MESH = pl.DeviceIdType.MESH
NB = 32
ROWS = 2 * NB
GX = 128
GY = 256
HALF = GX // 2
EXTRA = 3
CHUNK = 8
NCHUNK = HALF // CHUNK
TILE = 16
GROUP = 8
RELAYED = ((1,), (1,), (4, 5, 6, 7), (4, 5, 6, 7))
LATE = 4
PANEL = 4
F32 = jnp.float32
CONTRACT = (((1,), (1,)), ((), ()))


def dot(a, b):
    return lax.dot_general(a, b, CONTRACT, preferred_element_type=F32)


def complex_parts(square):
    real = square[:NB, :NB] + square[NB:, NB:]
    imag = square[:NB, NB:] - square[NB:, :NB]
    return real, imag


def product(a, b):
    return a[0] * b[0] - a[1] * b[1], a[0] * b[1] + a[1] * b[0]


def conjugate(a):
    return a[0], -a[1]


def less(a, b):
    return a[0] - b[0], a[1] - b[1]


def eliminate(tiles):
    tiles = [tuple(tile) for tile in tiles]
    pivots = [([], []) for _ in tiles]
    for start in range(0, NB, PANEL):
        count = tiles[0][0].shape[0]
        offset = start - (NB - count)
        lane = lax.broadcasted_iota(jnp.int32, (count, 128), 1)
        row_id = lax.broadcasted_iota(jnp.int32, (count, 128), 0)
        base = (lane // NB) * NB + start
        for n, work in enumerate(tiles):
            cols = [
                tuple(jnp.take_along_axis(w, base + e, axis=1) for w in work)
                for e in range(PANEL)
            ]
            rows = [tuple(w[offset + e : offset + e + 1] for w in work) for e in range(PANEL)]
            for e in range(PANEL):
                at = offset + e
                pivot = tuple(c[at : at + 1] for c in cols[e])
                for part in range(2):
                    pivots[n][part].append(pivot[part])
                if start + e == NB - 1:
                    break
                scale = 1.0 / (pivot[0] * pivot[0] + pivot[1] * pivot[1])
                factor = product(cols[e], (pivot[0] * scale, -pivot[1] * scale))
                factor = tuple(jnp.where(row_id > at, f, 0.0) for f in factor)
                for g in range(e + 1, PANEL):
                    cols[g] = less(cols[g], product(factor, [c[at : at + 1] for c in cols[g]]))
                    piece = [f[offset + g : offset + g + 1] for f in factor]
                    rows[g] = less(rows[g], product(piece, rows[e]))
                if start + PANEL < NB:
                    work = less(work, product(factor, rows[e]))
            drop = (offset + PANEL) // 8 * 8
            tiles[n] = tuple(w[drop:] for w in work)
    return [unit_product(*(jnp.concatenate(part, axis=0) for part in p)) for p in pivots]


def unit_product(pr, pi):
    mag = jnp.sqrt(pr * pr + pi * pi)
    ur = pr / mag
    ui = pi / mag
    n = NB
    while n > 1:
        n //= 2
        ar, ai, br, bi = ur[:n], ui[:n], ur[n:], ui[n:]
        ur, ui = ar * br - ai * bi, ar * bi + ai * br
    return ur, ui


def kernel(
    bands_in, umk_in, coeffs, flux, links,
    cv, perm, u, zm, zp, xp, xm, szm, szp, sxp, sxm, wb, xb,
    acc_a, acc_b, acc_d, left_src, left_dst, down_src, down_dst, corner_src, corner_dst,
    hop, load_sem, send_sem, recv_sem, ez_sem, part_sem, hop_sem,
    bands, umk, index_sem,
):
    i = lax.axis_index("kx")
    j = lax.axis_index("ky")
    ni = lax.axis_size("kx")
    nj = lax.axis_size("ky")
    right = (lax.rem(i + 1, ni), j)
    left = (lax.rem(i + ni - 1, ni), j)
    up = (i, lax.rem(j + 1, nj))
    down = (i, lax.rem(j + nj - 1, nj))
    x_edge = i == ni - 1
    y_edge = j == 0
    edge = jnp.logical_or(x_edge, y_edge)

    def load(t):
        rows = pl.ds(t * TILE, TILE)
        return pltpu.make_async_copy(coeffs.at[:, :, rows, :], cv[t], load_sem.at[t])

    half_tiles = HALF // TILE
    indices = [
        pltpu.make_async_copy(bands_in, bands, index_sem.at[0]),
        pltpu.make_async_copy(umk_in, umk, index_sem.at[1]),
    ]
    for copy in indices:
        copy.start()
    load(0).start()
    load(half_tiles).start()

    def shifted(di, dj):
        return lax.rem(i + di + ni, ni), lax.rem(j + dj + nj, nj)

    in_row = lax.rem(i, GROUP)
    in_column = lax.rem(j, GROUP)
    first_plane = in_column == 0
    last_plane = in_column == GROUP - 1
    wrap_plane = jnp.logical_or(first_plane, last_plane)
    sends_by = (
        first_plane,
        last_plane,
        jnp.logical_and(wrap_plane, in_row == GROUP - 1),
        jnp.logical_and(wrap_plane, in_row == 0),
    )
    relay_of = (shifted(0, -2), shifted(0, 2), shifted(5, 0), shifted(-5, 0))
    is_relay = (
        in_column == GROUP - 2,
        in_column == 1,
        jnp.logical_and(wrap_plane, in_row == 4),
        jnp.logical_and(wrap_plane, in_row == 3),
    )
    relay_from = (shifted(0, 2), shifted(0, -2), shifted(-5, 0), shifted(5, 0))
    relay_to = (up, down, shifted(-4, 0), shifted(4, 0))
    gets_by = (None, None, sends_by[3], sends_by[2])
    gets_from = (None, None, shifted(4, 0), shifted(-4, 0))

    barrier = pltpu.get_barrier_semaphore()
    for device in (right, left, up, down, shifted(1, 1), shifted(-1, -1)):
        pl.semaphore_signal(barrier, inc=1, device_id=device, device_id_type=MESH)
    arrivals = jnp.int32(6)
    for flags, devices in (
        (sends_by, relay_of),
        (is_relay, relay_from),
        ((None, None, *is_relay[2:]), relay_to),
        (gets_by, gets_from),
    ):
        for flag, device in zip(flags, devices, strict=True):
            if flag is None:
                continue
            arrivals = arrivals + jnp.where(flag, 1, 0)

            @pl.when(flag)
            def _(device=device):
                pl.semaphore_signal(barrier, inc=1, device_id=device, device_id_type=MESH)

    for copy in indices:
        copy.wait()
    zero = jnp.int32(0)
    ax = jnp.where(x_edge, umk[0, 0], zero)
    bx = jnp.where(x_edge, umk[0, 1], zero)
    ay = jnp.where(y_edge, umk[1, 0], zero)
    by = jnp.where(y_edge, umk[1, 1], zero)

    size = TILE * TILE
    to = lax.broadcasted_iota(jnp.int32, (size, size), 0)
    take = lax.broadcasted_iota(jnp.int32, (size, size), 1)
    swap = (to % TILE) * TILE + to // TILE
    perm[...] = jnp.where(take == swap, 1.0, 0.0).astype(jnp.bfloat16)

    acc_a[...] = jnp.zeros_like(acc_a)
    acc_b[...] = jnp.zeros_like(acc_b)
    acc_d[...] = jnp.zeros_like(acc_d)

    for t in range(1, half_tiles):
        load(t).start()
        load(t + half_tiles).start()

    def remote(src, dst, stream, c, device):
        return pltpu.make_async_remote_copy(
            src_ref=src, dst_ref=dst, send_sem=send_sem.at[stream, c],
            recv_sem=recv_sem.at[stream, c], device_id=device, device_id_type=MESH,
        )

    def stream_ends(stream, c, special):
        low = pl.ds(c * CHUNK, CHUNK)
        high = pl.ds(HALF + c * CHUNK, CHUNK)
        own, src, dst, device = (
            (low, szm, zm, down),
            (high, szp, zp, up),
            (low, sxp, xp, right),
            (high, sxm, xm, left),
        )[stream]
        source = src.at[low] if special else u.at[own]
        return source, dst.at[low], device

    def slot(stream, c):
        return pl.ds(RELAYED[stream].index(c) * CHUNK, CHUNK)

    def stream_wait(stream, c):
        return remote(*stream_ends(stream, c, False)[:2], stream, c, right)

    def stream_send(stream, c, special, when, first=False):
        source, target, device = stream_ends(stream, c, special)
        if first and stream < 2 and c >= LATE:
            when = jnp.logical_and(when, jnp.logical_not(is_relay[1 - stream]))
        if c not in RELAYED[stream]:

            @pl.when(when)
            def _():
                remote(source, target, stream, c, device).start()

            return

        @pl.when(jnp.logical_and(when, jnp.logical_not(sends_by[stream])))
        def _():
            remote(source, target, stream, c, device).start()

        @pl.when(jnp.logical_and(when, sends_by[stream]))
        def _():
            pltpu.make_async_remote_copy(
                src_ref=source, dst_ref=hop.at[slot(stream, c)],
                send_sem=send_sem.at[stream, c], recv_sem=hop_sem.at[0, c],
                device_id=relay_of[stream], device_id_type=MESH,
            ).start()

    def relay_copy(stream, c):
        source = hop.at[slot(stream, c)]
        target = stream_ends(stream, c, False)[1]
        return pltpu.make_async_remote_copy(
            src_ref=source, dst_ref=target, send_sem=hop_sem.at[1, c],
            recv_sem=recv_sem.at[stream, c], device_id=relay_to[stream],
            device_id_type=MESH,
        )

    def relay_arrival(stream, c):
        rows = hop.at[slot(stream, c)]
        return pltpu.make_async_remote_copy(
            src_ref=rows, dst_ref=rows, send_sem=hop_sem.at[1, c],
            recv_sem=hop_sem.at[0, c], device_id=right, device_id_type=MESH,
        )

    need = (y_edge, x_edge, x_edge, y_edge)

    def gather(t):
        rows = pl.ds(t * TILE, TILE)
        for g in range(ROWS // TILE):
            r, b = divmod(g * TILE, NB)
            parts = [cv[t][r, bands[b + e]] for e in range(TILE)]
            moved = jnp.dot(perm[...], jnp.concatenate(parts, axis=0), preferred_element_type=F32)
            moved = moved.astype(jnp.bfloat16).reshape(TILE, TILE, GY)
            u[rows, pl.ds(g * TILE, TILE), :] = moved

    for t in range(half_tiles):
        load(t).wait()
        gather(t)
        load(t + half_tiles).wait()
        gather(t + half_tiles)
        if t == 0:
            pl.semaphore_wait(barrier, arrivals)
        for c in range(t * TILE // CHUNK, (t + 1) * TILE // CHUNK):
            for stream in range(4):
                stream_send(stream, c, False, jnp.logical_not(need[stream]), True)

    def build(dst, count, first, dp, dq):
        shift = lax.rem(GY - dq, GY)

        @pl.loop(0, count // 8)
        def _(c):
            for q in range(8):
                p = c * 8 + q
                row = lax.rem(first + p + dp + GX, GX)
                dst[p] = pltpu.roll(u[row], shift, 1)

    def build_extra(dst, forward, dq):
        shift = lax.rem(GY - dq, GY)
        for e in range(EXTRA):
            row = jnp.where(forward, e, HALF - EXTRA + e)
            dst[HALF + e] = pltpu.roll(u[row], shift, 1)

    def extra(stream, src, dst, device):
        rows = pl.ds(HALF, EXTRA)
        return pltpu.make_async_remote_copy(
            src_ref=src.at[rows], dst_ref=dst.at[rows], send_sem=ez_sem.at[0, stream],
            recv_sem=ez_sem.at[1, stream], device_id=device, device_id_type=MESH,
        )

    @pl.when(y_edge)
    def _():
        build(szm, HALF, 0, -ay, -by)
        for c in range(NCHUNK):
            stream_send(0, c, True, True, True)

    @pl.when(x_edge)
    def _():
        build(szp, HALF, HALF, 0, bx)
        build_extra(szp, ax > 0, bx)
        extra(0, szp, zp, up).start()
        for c in range(NCHUNK):
            stream_send(1, c, True, True, True)
        build(sxp, HALF, 0, ax, bx)
        for c in range(NCHUNK):
            stream_send(2, c, True, True, True)

    @pl.when(y_edge)
    def _():
        build(sxm, HALF, HALF, 0, -by)
        build_extra(sxm, ay < 0, -by)
        extra(1, sxm, xm, left).start()
        for c in range(NCHUNK):
            stream_send(3, c, True, True, True)

    for stream in range(4):

        @pl.when(is_relay[stream])
        def _(stream=stream):
            for c in RELAYED[stream]:
                relay_arrival(stream, c).wait_recv()
                relay_copy(stream, c).start()
            if stream < 2:
                other = 1 - stream
                for c in range(LATE, NCHUNK):
                    stream_send(other, c, False, jnp.logical_not(need[other]))
                    stream_send(other, c, True, need[other])

    build(wb, HALF, HALF, -ay, bx - by)
    build(xb, HALF, HALF, ax, bx - by)

    @pl.loop(0, NCHUNK)
    def _(step):
        early, late = RELAYED[0][0], len(RELAYED[0])
        turn = NCHUNK - 1 - late
        c = jnp.where(step < early, step, step + late)
        c = jnp.where(step < turn, c, early + step - turn)
        c = jnp.where(step == NCHUNK - 1, step, c)
        for stream in range(4):
            stream_wait(stream, c).wait_recv()
        first = c * CHUNK
        a = None
        b = None
        for q in range(CHUNK):
            p = first + q
            own = u[p]
            lhs = jnp.concatenate([own, xp[p]], axis=0)
            rhs = jnp.concatenate([zm[p], own], axis=0)
            term = dot(lhs, rhs)
            a = term if a is None else a + term
            lhs = jnp.concatenate([zp[p], xb[p]], axis=0)
            rhs = jnp.concatenate([wb[p], xm[p]], axis=0)
            term = dot(lhs, rhs)
            b = term if b is None else b + term
        acc_a[...] += a
        acc_b[...] += b

    acc_d[...] = acc_b[:ROWS, ROWS:]

    @pl.when(x_edge)
    def _():
        extra(0, szp, zp, up).wait_recv()

    @pl.when(y_edge)
    def _():
        extra(1, sxm, xm, left).wait_recv()

    @pl.when(edge)
    def _():
        acc_d[...] = jnp.zeros_like(acc_d)

        @pl.loop(0, HALF // 32)
        def _(c):
            total = None
            for q in range(32):
                s = c * 32 + q + ax
                t = c * 32 + q - ay
                s = jnp.where(s < 0, s + HALF + EXTRA, s)
                t = jnp.where(t < 0, t + HALF + EXTRA, t)
                term = dot(zp[s], xm[t])
                total = term if total is None else total + term
            acc_d[...] += total

    a = acc_a[...]
    b = acc_b[...]
    d_low = complex_parts(a[ROWS:, :ROWS])
    x_low = complex_parts(a[ROWS:, ROWS:])
    y_low = complex_parts(a[:ROWS, :ROWS])
    y_high = complex_parts(b[:ROWS, :ROWS])
    x_high = complex_parts(b[ROWS:, ROWS:])
    d_high = complex_parts(acc_d[...])
    none = jnp.zeros((NB, NB), F32)

    lane = lax.broadcasted_iota(jnp.int32, (NB, 128), 1)
    low, high = [], []
    for part in range(2):
        rows = pl.ds(part * NB, NB)
        low.append(jnp.concatenate([x_low[part], y_low[part], d_low[part], none], axis=1))
        high.append(jnp.concatenate([x_high[part], y_high[part], d_high[part], none], axis=1))
        left_src[rows, :] = low[part]
        down_src[rows, :] = high[part]
        corner_src[rows, :] = jnp.where(lane < NB, low[part], high[part])

    def part_copy(which):
        src, dst, device = (
            (left_src, left_dst, left),
            (down_src, down_dst, down),
            (corner_src, corner_dst, shifted(-1, -1)),
        )[which]
        return pltpu.make_async_remote_copy(
            src_ref=src, dst_ref=dst, send_sem=part_sem.at[0, which],
            recv_sem=part_sem.at[1, which], device_id=device, device_id_type=MESH,
        )

    for which in (2, 1, 0):
        part_copy(which).start()
    for which in range(3):
        part_copy(which).wait_recv()
    own_tile, next_tile = [], []
    for part in range(2):
        rows = pl.ds(part * NB, NB)
        of_left, of_down, of_corner = left_dst[rows, :], down_dst[rows, :], corner_dst[rows, :]
        other = jnp.where(lane < 2 * NB, low[part] + of_down, of_left + of_down)
        other = jnp.where(lane < NB, high[part] + of_left, other)
        own_tile.append(jnp.where(lane < 3 * NB, other, 1.0))
        other = of_corner + jnp.where(lane < NB, of_down, of_left)
        next_tile.append(jnp.where(lane < 2 * NB, other, 1.0))
    unit, unit_next = eliminate((own_tile, next_tile))

    def group(ref, which):
        real, imag = ref
        if which:
            shift = 128 - which * NB
            real, imag = pltpu.roll(real, shift, 1), pltpu.roll(imag, shift, 1)
        return real, imag

    along_x, along_y, along_d = (group(unit, which) for which in range(3))
    y_next = group(unit_next, 1)
    x_next = group(unit_next, 0)
    first = product(product(along_x, y_next), conjugate(along_d))
    second = product(product(along_d, conjugate(x_next)), conjugate(along_y))
    lane = lax.broadcasted_iota(jnp.int32, (1, 128), 1)
    angle = jnp.arctan2(
        jnp.where(lane == 0, first[1], second[1]), jnp.where(lane == 0, first[0], second[0])
    )
    flux[0] = angle[:, :2]
    for part in range(2):
        row = jnp.where(lane == 0, along_x[part], along_y[part])
        row = jnp.where(lane == 2, along_d[part], row)
        links[0, 0, part : part + 1, :] = row[:, :3]

    @pl.loop(0, NCHUNK)
    def _(c):
        for stream in range(4):
            stream_wait(stream, c).wait_send()

    @pl.when(x_edge)
    def _():
        extra(0, szp, zp, up).wait_send()

    @pl.when(y_edge)
    def _():
        extra(1, sxm, xm, left).wait_send()

    for stream in range(4):

        @pl.when(is_relay[stream])
        def _(stream=stream):
            for c in RELAYED[stream]:
                relay_copy(stream, c).wait_send()

    for which in range(3):
        part_copy(which).wait_send()


def per_device(coeffs, bands, umklapp):
    bf16 = jnp.bfloat16
    half = pltpu.VMEM((HALF, ROWS, GY), bf16)
    longer = pltpu.VMEM((HALF + EXTRA, ROWS, GY), bf16)
    flux, links = pl.pallas_call(
        kernel,
        out_shape=(
            jax.ShapeDtypeStruct((1, 1, 2), F32),
            jax.ShapeDtypeStruct((1, 1, 2, 3), F32),
        ),
        in_specs=[
            pl.BlockSpec(memory_space=pltpu.HBM),
            pl.BlockSpec(memory_space=pltpu.HBM),
            pl.BlockSpec(memory_space=pltpu.HBM),
        ],
        out_specs=(pl.BlockSpec(memory_space=pltpu.VMEM),) * 2,
        scratch_shapes=[
            [pltpu.VMEM((*coeffs.shape[2:4], TILE, GY), bf16)] * (GX // TILE),
            pltpu.VMEM((TILE * TILE, TILE * TILE), bf16),
            pltpu.VMEM((GX, ROWS, GY), bf16),
            half, longer, half, longer,
            half, longer, half, longer, half, half,
            pltpu.VMEM((2 * ROWS, 2 * ROWS), F32),
            pltpu.VMEM((2 * ROWS, 2 * ROWS), F32),
            pltpu.VMEM((ROWS, ROWS), F32),
            pltpu.VMEM((ROWS, 128), F32),
            pltpu.VMEM((ROWS, 128), F32),
            pltpu.VMEM((ROWS, 128), F32),
            pltpu.VMEM((ROWS, 128), F32),
            pltpu.VMEM((ROWS, 128), F32),
            pltpu.VMEM((ROWS, 128), F32),
            pltpu.VMEM((max(map(len, RELAYED)) * CHUNK, ROWS, GY), bf16),
            pltpu.SemaphoreType.DMA((GX // TILE,)),
            pltpu.SemaphoreType.DMA((4, NCHUNK)),
            pltpu.SemaphoreType.DMA((4, NCHUNK)),
            pltpu.SemaphoreType.DMA((2, 2)),
            pltpu.SemaphoreType.DMA((2, 3)),
            pltpu.SemaphoreType.DMA((2, NCHUNK)),
            pltpu.SMEM((NB,), jnp.int32),
            pltpu.SMEM((2, 2), jnp.int32),
            pltpu.SemaphoreType.DMA((2,)),
        ],
        compiler_params=pltpu.CompilerParams(
            collective_id=0, has_side_effects=True, vmem_limit_bytes=50 << 20
        ),
    )(*(pltpu.with_memory_space_constraint(v, pltpu.HBM) for v in (bands, umklapp, coeffs[0, 0])))
    return flux, jnp.swapaxes(links, 2, 3)


def solution(mesh):
    in_specs = (P("kx", "ky", None, None, None, None), P(), P())
    out_specs = (P("kx", "ky", None), P("kx", "ky", None, None))
    return jax.shard_map(
        per_device, mesh=mesh, in_specs=in_specs, out_specs=out_specs, check_vma=False
    )
```

```python
import functools

import jax
import jax.numpy as jnp
from jax import lax
from jax.experimental import pallas as pl
from jax.experimental.pallas import tpu as pltpu
from jax.sharding import PartitionSpec as P

MESH = pl.DeviceIdType.MESH
NB = 32
ROWS = 2 * NB
GX = 128
GY = 256
HALF = GX // 2
EXTRA = 3
CHUNK = 8
NCHUNK = HALF // CHUNK
TILE = 16
GROUP = 8
RELAYED = ((1,), (1,), (4, 5, 6, 7), (4, 5, 6, 7))
LATE = 4
PANEL = 4
F32 = jnp.float32
CONTRACT = (((1,), (1,)), ((), ()))


def dot(a, b):
    return lax.dot_general(a, b, CONTRACT, preferred_element_type=F32)


def complex_parts(square):
    real = square[:NB, :NB] + square[NB:, NB:]
    imag = square[:NB, NB:] - square[NB:, :NB]
    return real, imag


def product(a, b):
    return a[0] * b[0] - a[1] * b[1], a[0] * b[1] + a[1] * b[0]


def conjugate(a):
    return a[0], -a[1]


def less(a, b):
    return a[0] - b[0], a[1] - b[1]


def eliminate(tiles):
    tiles = [tuple(tile) for tile in tiles]
    pivots = [([], []) for _ in tiles]
    for start in range(0, NB, PANEL):
        count = tiles[0][0].shape[0]
        offset = start - (NB - count)
        lane = lax.broadcasted_iota(jnp.int32, (count, 128), 1)
        row_id = lax.broadcasted_iota(jnp.int32, (count, 128), 0)
        base = (lane // NB) * NB + start
        for n, work in enumerate(tiles):
            cols = [
                tuple(jnp.take_along_axis(w, base + e, axis=1) for w in work)
                for e in range(PANEL)
            ]
            rows = [tuple(w[offset + e : offset + e + 1] for w in work) for e in range(PANEL)]
            for e in range(PANEL):
                at = offset + e
                pivot = tuple(c[at : at + 1] for c in cols[e])
                for part in range(2):
                    pivots[n][part].append(pivot[part])
                if start + e == NB - 1:
                    break
                scale = 1.0 / (pivot[0] * pivot[0] + pivot[1] * pivot[1])
                factor = product(cols[e], (pivot[0] * scale, -pivot[1] * scale))
                factor = tuple(jnp.where(row_id > at, f, 0.0) for f in factor)
                for g in range(e + 1, PANEL):
                    cols[g] = less(cols[g], product(factor, [c[at : at + 1] for c in cols[g]]))
                    piece = [f[offset + g : offset + g + 1] for f in factor]
                    rows[g] = less(rows[g], product(piece, rows[e]))
                if start + PANEL < NB:
                    work = less(work, product(factor, rows[e]))
            drop = (offset + PANEL) // 8 * 8
            tiles[n] = tuple(w[drop:] for w in work)
    return [unit_product(*(jnp.concatenate(part, axis=0) for part in p)) for p in pivots]


def unit_product(pr, pi):
    mag = jnp.sqrt(pr * pr + pi * pi)
    ur = pr / mag
    ui = pi / mag
    n = NB
    while n > 1:
        n //= 2
        ar, ai, br, bi = ur[:n], ui[:n], ur[n:], ui[n:]
        ur, ui = ar * br - ai * bi, ar * bi + ai * br
    return ur, ui


def kernel(
    bands_in, umk_in, coeffs, flux, links,
    cv, perm, u, zm, zp, xp, xm, szm, szp, sxp, sxm, wb, xb,
    acc_a, acc_b, acc_d, left_src, left_dst, down_src, down_dst, corner_src, corner_dst,
    hop, load_sem, send_sem, recv_sem, ez_sem, part_sem, hop_sem,
    bands, umk, index_sem,
):
    i = lax.axis_index("kx")
    j = lax.axis_index("ky")
    ni = lax.axis_size("kx")
    nj = lax.axis_size("ky")
    right = (lax.rem(i + 1, ni), j)
    left = (lax.rem(i + ni - 1, ni), j)
    up = (i, lax.rem(j + 1, nj))
    down = (i, lax.rem(j + nj - 1, nj))
    x_edge = i == ni - 1
    y_edge = j == 0
    edge = jnp.logical_or(x_edge, y_edge)

    def load(t):
        rows = pl.ds(t * TILE, TILE)
        return pltpu.make_async_copy(coeffs.at[:, :, rows, :], cv[t], load_sem.at[t])

    half_tiles = HALF // TILE
    indices = [
        pltpu.make_async_copy(bands_in, bands, index_sem.at[0]),
        pltpu.make_async_copy(umk_in, umk, index_sem.at[1]),
    ]
    for copy in indices:
        copy.start()
    load(0).start()
    load(half_tiles).start()

    def shifted(di, dj):
        return lax.rem(i + di + ni, ni), lax.rem(j + dj + nj, nj)

    in_row = lax.rem(i, GROUP)
    in_column = lax.rem(j, GROUP)
    first_plane = in_column == 0
    last_plane = in_column == GROUP - 1
    wrap_plane = jnp.logical_or(first_plane, last_plane)
    sends_by = (
        first_plane,
        last_plane,
        jnp.logical_and(wrap_plane, in_row == GROUP - 1),
        jnp.logical_and(wrap_plane, in_row == 0),
    )
    relay_of = (shifted(0, -2), shifted(0, 2), shifted(5, 0), shifted(-5, 0))
    is_relay = (
        in_column == GROUP - 2,
        in_column == 1,
        jnp.logical_and(wrap_plane, in_row == 4),
        jnp.logical_and(wrap_plane, in_row == 3),
    )
    relay_from = (shifted(0, 2), shifted(0, -2), shifted(-5, 0), shifted(5, 0))
    relay_to = (up, down, shifted(-4, 0), shifted(4, 0))
    gets_by = (None, None, sends_by[3], sends_by[2])
    gets_from = (None, None, shifted(4, 0), shifted(-4, 0))

    barrier = pltpu.get_barrier_semaphore()
    for device in (right, left, up, down, shifted(1, 1), shifted(-1, -1)):
        pl.semaphore_signal(barrier, inc=1, device_id=device, device_id_type=MESH)
    arrivals = jnp.int32(6)
    for flags, devices in (
        (sends_by, relay_of),
        (is_relay, relay_from),
        ((None, None, *is_relay[2:]), relay_to),
        (gets_by, gets_from),
    ):
        for flag, device in zip(flags, devices, strict=True):
            if flag is None:
                continue
            arrivals = arrivals + jnp.where(flag, 1, 0)

            @pl.when(flag)
            def _(device=device):
                pl.semaphore_signal(barrier, inc=1, device_id=device, device_id_type=MESH)

    for copy in indices:
        copy.wait()
    zero = jnp.int32(0)
    ax = jnp.where(x_edge, umk[0, 0], zero)
    bx = jnp.where(x_edge, umk[0, 1], zero)
    ay = jnp.where(y_edge, umk[1, 0], zero)
    by = jnp.where(y_edge, umk[1, 1], zero)

    size = TILE * TILE
    to = lax.broadcasted_iota(jnp.int32, (size, size), 0)
    take = lax.broadcasted_iota(jnp.int32, (size, size), 1)
    swap = (to % TILE) * TILE + to // TILE
    perm[...] = jnp.where(take == swap, 1.0, 0.0).astype(jnp.bfloat16)

    acc_a[...] = jnp.zeros_like(acc_a)
    acc_b[...] = jnp.zeros_like(acc_b)
    acc_d[...] = jnp.zeros_like(acc_d)

    for t in range(1, half_tiles):
        load(t).start()
        load(t + half_tiles).start()

    def remote(src, dst, stream, c, device):
        return pltpu.make_async_remote_copy(
            src_ref=src, dst_ref=dst, send_sem=send_sem.at[stream, c],
            recv_sem=recv_sem.at[stream, c], device_id=device, device_id_type=MESH,
        )

    def stream_ends(stream, c, special):
        low = pl.ds(c * CHUNK, CHUNK)
        high = pl.ds(HALF + c * CHUNK, CHUNK)
        own, src, dst, device = (
            (low, szm, zm, down),
            (high, szp, zp, up),
            (low, sxp, xp, right),
            (high, sxm, xm, left),
        )[stream]
        source = src.at[low] if special else u.at[own]
        return source, dst.at[low], device

    def slot(stream, c):
        return pl.ds(RELAYED[stream].index(c) * CHUNK, CHUNK)

    def stream_wait(stream, c):
        return remote(*stream_ends(stream, c, False)[:2], stream, c, right)

    def stream_send(stream, c, special, when, first=False):
        source, target, device = stream_ends(stream, c, special)
        if first and stream < 2 and c >= LATE:
            when = jnp.logical_and(when, jnp.logical_not(is_relay[1 - stream]))
        if c not in RELAYED[stream]:

            @pl.when(when)
            def _():
                remote(source, target, stream, c, device).start()

            return

        @pl.when(jnp.logical_and(when, jnp.logical_not(sends_by[stream])))
        def _():
            remote(source, target, stream, c, device).start()

        @pl.when(jnp.logical_and(when, sends_by[stream]))
        def _():
            pltpu.make_async_remote_copy(
                src_ref=source, dst_ref=hop.at[slot(stream, c)],
                send_sem=send_sem.at[stream, c], recv_sem=hop_sem.at[0, c],
                device_id=relay_of[stream], device_id_type=MESH,
            ).start()

    def relay_copy(stream, c):
        source = hop.at[slot(stream, c)]
        target = stream_ends(stream, c, False)[1]
        return pltpu.make_async_remote_copy(
            src_ref=source, dst_ref=target, send_sem=hop_sem.at[1, c],
            recv_sem=recv_sem.at[stream, c], device_id=relay_to[stream],
            device_id_type=MESH,
        )

    def relay_arrival(stream, c):
        rows = hop.at[slot(stream, c)]
        return pltpu.make_async_remote_copy(
            src_ref=rows, dst_ref=rows, send_sem=hop_sem.at[1, c],
            recv_sem=hop_sem.at[0, c], device_id=right, device_id_type=MESH,
        )

    need = (y_edge, x_edge, x_edge, y_edge)

    def gather(t):
        rows = pl.ds(t * TILE, TILE)
        for g in range(ROWS // TILE):
            r, b = divmod(g * TILE, NB)
            parts = [cv[t][r, bands[b + e]] for e in range(TILE)]
            moved = jnp.dot(perm[...], jnp.concatenate(parts, axis=0), preferred_element_type=F32)
            moved = moved.astype(jnp.bfloat16).reshape(TILE, TILE, GY)
            u[rows, pl.ds(g * TILE, TILE), :] = moved

    for t in range(half_tiles):
        load(t).wait()
        gather(t)
        load(t + half_tiles).wait()
        gather(t + half_tiles)
        if t == 0:
            pl.semaphore_wait(barrier, arrivals)
        for c in range(t * TILE // CHUNK, (t + 1) * TILE // CHUNK):
            for stream in range(4):
                stream_send(stream, c, False, jnp.logical_not(need[stream]), True)

    def build(dst, count, first, dp, dq):
        shift = lax.rem(GY - dq, GY)

        @pl.loop(0, count // 8)
        def _(c):
            for q in range(8):
                p = c * 8 + q
                row = lax.rem(first + p + dp + GX, GX)
                dst[p] = pltpu.roll(u[row], shift, 1)

    def build_extra(dst, forward, dq):
        shift = lax.rem(GY - dq, GY)
        for e in range(EXTRA):
            row = jnp.where(forward, e, HALF - EXTRA + e)
            dst[HALF + e] = pltpu.roll(u[row], shift, 1)

    def extra(stream, src, dst, device):
        rows = pl.ds(HALF, EXTRA)
        return pltpu.make_async_remote_copy(
            src_ref=src.at[rows], dst_ref=dst.at[rows], send_sem=ez_sem.at[0, stream],
            recv_sem=ez_sem.at[1, stream], device_id=device, device_id_type=MESH,
        )

    @pl.when(y_edge)
    def _():
        build(szm, HALF, 0, -ay, -by)
        for c in range(NCHUNK):
            stream_send(0, c, True, True, True)

    @pl.when(x_edge)
    def _():
        build(szp, HALF, HALF, 0, bx)
        build_extra(szp, ax > 0, bx)
        extra(0, szp, zp, up).start()
        for c in range(NCHUNK):
            stream_send(1, c, True, True, True)
        build(sxp, HALF, 0, ax, bx)
        for c in range(NCHUNK):
            stream_send(2, c, True, True, True)

    @pl.when(y_edge)
    def _():
        build(sxm, HALF, HALF, 0, -by)
        build_extra(sxm, ay < 0, -by)
        extra(1, sxm, xm, left).start()
        for c in range(NCHUNK):
            stream_send(3, c, True, True, True)

    for stream in range(4):

        @pl.when(is_relay[stream])
        def _(stream=stream):
            for c in RELAYED[stream]:
                relay_arrival(stream, c).wait_recv()
                relay_copy(stream, c).start()
            if stream < 2:
                other = 1 - stream
                for c in range(LATE, NCHUNK):
                    stream_send(other, c, False, jnp.logical_not(need[other]))
                    stream_send(other, c, True, need[other])

    build(wb, HALF, HALF, -ay, bx - by)
    build(xb, HALF, HALF, ax, bx - by)

    def diagonal(place, row, count):
        total = None
        for q in range(count):
            source = row + q - ax
            inside = jnp.logical_and(source >= 0, source < HALF)
            target = jnp.where(inside, source - ay, 0)
            target = jnp.where(target < 0, target + HALF + EXTRA, target)
            left_rows = zp[place + q]
            term = dot(jnp.where(inside, left_rows, jnp.zeros_like(left_rows)), xm[target])
            total = term if total is None else total + term
        acc_d[...] += total

    @pl.when(edge)
    def _():
        for c in range(NCHUNK):
            stream_wait(3, c).wait_recv()

    @pl.when(y_edge)
    def _():
        extra(1, sxm, xm, left).wait_recv()

    @pl.when(x_edge)
    def _():
        extra(0, szp, zp, up).wait_recv()
        diagonal(HALF, jnp.where(ax > 0, HALF, -EXTRA), EXTRA)

    def low_terms(c):
        stream_wait(0, c).wait_recv()
        stream_wait(2, c).wait_recv()
        total = None
        for q in range(CHUNK):
            p = c * CHUNK + q
            own = u[p]
            term = dot(
                jnp.concatenate([own, xp[p]], axis=0), jnp.concatenate([zm[p], own], axis=0)
            )
            total = term if total is None else total + term
        acc_a[...] += total

    def high_terms(c):
        stream_wait(1, c).wait_recv()

        @pl.when(jnp.logical_not(edge))
        def _():
            stream_wait(3, c).wait_recv()

        total = None
        for q in range(CHUNK):
            p = c * CHUNK + q
            term = dot(
                jnp.concatenate([zp[p], xb[p]], axis=0), jnp.concatenate([wb[p], xm[p]], axis=0)
            )
            total = term if total is None else total + term
        acc_b[...] += total

        @pl.when(edge)
        def _():
            diagonal(c * CHUNK, c * CHUNK, CHUNK)

    @pl.loop(0, NCHUNK - 1)
    def _(step):
        early, late = RELAYED[0][0], len(RELAYED[0])
        turn = NCHUNK - 1 - late
        c = jnp.where(step < early, step, step + late)
        c = jnp.where(step < turn, c, early + step - turn)
        low_terms(c)
        high_terms(c)

    none = jnp.zeros((NB, NB), F32)

    def table(x, y, d):
        return [jnp.concatenate([x[part], y[part], d[part], none], axis=1) for part in range(2)]

    def part_copy(which):
        src, dst, device = (
            (left_src, left_dst, left),
            (down_src, down_dst, down),
            (corner_src, corner_dst, shifted(-1, -1)),
        )[which]
        return pltpu.make_async_remote_copy(
            src_ref=src, dst_ref=dst, send_sem=part_sem.at[0, which],
            recv_sem=part_sem.at[1, which], device_id=device, device_id_type=MESH,
        )

    low_terms(NCHUNK - 1)
    a = acc_a[...]
    low = table(
        complex_parts(a[ROWS:, ROWS:]),
        complex_parts(a[:ROWS, :ROWS]),
        complex_parts(a[ROWS:, :ROWS]),
    )
    for part in range(2):
        left_src[pl.ds(part * NB, NB), :] = low[part]
    part_copy(0).start()

    high_terms(NCHUNK - 1)

    @pl.when(jnp.logical_not(edge))
    def _():
        acc_d[...] = acc_b[:ROWS, ROWS:]

    b = acc_b[...]
    high = table(
        complex_parts(b[ROWS:, ROWS:]),
        complex_parts(b[:ROWS, :ROWS]),
        complex_parts(acc_d[...]),
    )
    lane = lax.broadcasted_iota(jnp.int32, (NB, 128), 1)
    for part in range(2):
        rows = pl.ds(part * NB, NB)
        down_src[rows, :] = high[part]
        corner_src[rows, :] = jnp.where(lane < NB, left_src[rows, :], high[part])
    part_copy(1).start()
    part_copy(2).start()
    for which in range(3):
        part_copy(which).wait_recv()
    own_tile, next_tile = [], []
    for part in range(2):
        rows = pl.ds(part * NB, NB)
        of_left, of_down, of_corner = left_dst[rows, :], down_dst[rows, :], corner_dst[rows, :]
        other = jnp.where(lane < 2 * NB, left_src[rows, :] + of_down, of_left + of_down)
        other = jnp.where(lane < NB, high[part] + of_left, other)
        own_tile.append(jnp.where(lane < 3 * NB, other, 1.0))
        other = of_corner + jnp.where(lane < NB, of_down, of_left)
        next_tile.append(jnp.where(lane < 2 * NB, other, 1.0))
    unit, unit_next = eliminate((own_tile, next_tile))

    def group(ref, which):
        real, imag = ref
        if which:
            shift = 128 - which * NB
            real, imag = pltpu.roll(real, shift, 1), pltpu.roll(imag, shift, 1)
        return real, imag

    along_x, along_y, along_d = (group(unit, which) for which in range(3))
    y_next = group(unit_next, 1)
    x_next = group(unit_next, 0)
    first = product(product(along_x, y_next), conjugate(along_d))
    second = product(product(along_d, conjugate(x_next)), conjugate(along_y))
    lane = lax.broadcasted_iota(jnp.int32, (1, 128), 1)
    angle = jnp.arctan2(
        jnp.where(lane == 0, first[1], second[1]), jnp.where(lane == 0, first[0], second[0])
    )
    flux[0] = angle[:, :2]
    for part in range(2):
        row = jnp.where(lane == 0, along_x[part], along_y[part])
        row = jnp.where(lane == 2, along_d[part], row)
        links[0, 0, part : part + 1, :] = row[:, :3]

    @pl.loop(0, NCHUNK)
    def _(c):
        for stream in range(4):
            stream_wait(stream, c).wait_send()

    @pl.when(x_edge)
    def _():
        extra(0, szp, zp, up).wait_send()

    @pl.when(y_edge)
    def _():
        extra(1, sxm, xm, left).wait_send()

    for stream in range(4):

        @pl.when(is_relay[stream])
        def _(stream=stream):
            for c in RELAYED[stream]:
                relay_copy(stream, c).wait_send()

    for which in range(3):
        part_copy(which).wait_send()


def per_device(coeffs, bands, umklapp):
    bf16 = jnp.bfloat16
    half = pltpu.VMEM((HALF, ROWS, GY), bf16)
    longer = pltpu.VMEM((HALF + EXTRA, ROWS, GY), bf16)
    flux, links = pl.pallas_call(
        kernel,
        out_shape=(
            jax.ShapeDtypeStruct((1, 1, 2), F32),
            jax.ShapeDtypeStruct((1, 1, 2, 3), F32),
        ),
        in_specs=[
            pl.BlockSpec(memory_space=pltpu.HBM),
            pl.BlockSpec(memory_space=pltpu.HBM),
            pl.BlockSpec(memory_space=pltpu.HBM),
        ],
        out_specs=(pl.BlockSpec(memory_space=pltpu.VMEM),) * 2,
        scratch_shapes=[
            [pltpu.VMEM((*coeffs.shape[2:4], TILE, GY), bf16)] * (GX // TILE),
            pltpu.VMEM((TILE * TILE, TILE * TILE), bf16),
            pltpu.VMEM((GX, ROWS, GY), bf16),
            half, longer, half, longer,
            half, longer, half, longer, half, half,
            pltpu.VMEM((2 * ROWS, 2 * ROWS), F32),
            pltpu.VMEM((2 * ROWS, 2 * ROWS), F32),
            pltpu.VMEM((ROWS, ROWS), F32),
            pltpu.VMEM((ROWS, 128), F32),
            pltpu.VMEM((ROWS, 128), F32),
            pltpu.VMEM((ROWS, 128), F32),
            pltpu.VMEM((ROWS, 128), F32),
            pltpu.VMEM((ROWS, 128), F32),
            pltpu.VMEM((ROWS, 128), F32),
            pltpu.VMEM((max(map(len, RELAYED)) * CHUNK, ROWS, GY), bf16),
            pltpu.SemaphoreType.DMA((GX // TILE,)),
            pltpu.SemaphoreType.DMA((4, NCHUNK)),
            pltpu.SemaphoreType.DMA((4, NCHUNK)),
            pltpu.SemaphoreType.DMA((2, 2)),
            pltpu.SemaphoreType.DMA((2, 3)),
            pltpu.SemaphoreType.DMA((2, NCHUNK)),
            pltpu.SMEM((NB,), jnp.int32),
            pltpu.SMEM((2, 2), jnp.int32),
            pltpu.SemaphoreType.DMA((2,)),
        ],
        compiler_params=pltpu.CompilerParams(
            collective_id=0, has_side_effects=True, vmem_limit_bytes=50 << 20
        ),
    )(*(pltpu.with_memory_space_constraint(v, pltpu.HBM) for v in (bands, umklapp, coeffs[0, 0])))
    return flux, jnp.swapaxes(links, 2, 3)


def solution(mesh):
    in_specs = (P("kx", "ky", None, None, None, None), P(), P())
    out_specs = (P("kx", "ky", None), P("kx", "ky", None, None))
    return jax.shard_map(
        per_device, mesh=mesh, in_specs=in_specs, out_specs=out_specs, check_vma=False
    )
```

```python
import functools

import jax
import jax.numpy as jnp
from jax import lax
from jax.experimental import pallas as pl
from jax.experimental.pallas import tpu as pltpu
from jax.sharding import PartitionSpec as P

MESH = pl.DeviceIdType.MESH
NB = 32
ROWS = 2 * NB
GX = 128
GY = 256
HALF = GX // 2
EXTRA = 3
CHUNK = 8
NCHUNK = HALF // CHUNK
TILE = 16
GROUP = 8
RELAYED = ((1,), (1,), (4, 5, 6, 7), (4, 5, 6, 7))
LATE = 5
PANEL = 4
F32 = jnp.float32
CONTRACT = (((1,), (1,)), ((), ()))


def dot(a, b):
    return lax.dot_general(a, b, CONTRACT, preferred_element_type=F32)


def complex_parts(square):
    real = square[:NB, :NB] + square[NB:, NB:]
    imag = square[:NB, NB:] - square[NB:, :NB]
    return real, imag


def product(a, b):
    return a[0] * b[0] - a[1] * b[1], a[0] * b[1] + a[1] * b[0]


def conjugate(a):
    return a[0], -a[1]


def less(a, b):
    return a[0] - b[0], a[1] - b[1]


def eliminate(tiles):
    tiles = [tuple(tile) for tile in tiles]
    pivots = [([], []) for _ in tiles]
    for start in range(0, NB, PANEL):
        count = tiles[0][0].shape[0]
        offset = start - (NB - count)
        lane = lax.broadcasted_iota(jnp.int32, (count, 128), 1)
        row_id = lax.broadcasted_iota(jnp.int32, (count, 128), 0)
        base = (lane // NB) * NB + start
        for n, work in enumerate(tiles):
            cols = [
                tuple(jnp.take_along_axis(w, base + e, axis=1) for w in work)
                for e in range(PANEL)
            ]
            rows = [tuple(w[offset + e : offset + e + 1] for w in work) for e in range(PANEL)]
            for e in range(PANEL):
                at = offset + e
                pivot = tuple(c[at : at + 1] for c in cols[e])
                for part in range(2):
                    pivots[n][part].append(pivot[part])
                if start + e == NB - 1:
                    break
                scale = 1.0 / (pivot[0] * pivot[0] + pivot[1] * pivot[1])
                factor = product(cols[e], (pivot[0] * scale, -pivot[1] * scale))
                factor = tuple(jnp.where(row_id > at, f, 0.0) for f in factor)
                for g in range(e + 1, PANEL):
                    cols[g] = less(cols[g], product(factor, [c[at : at + 1] for c in cols[g]]))
                    piece = [f[offset + g : offset + g + 1] for f in factor]
                    rows[g] = less(rows[g], product(piece, rows[e]))
                if start + PANEL < NB:
                    work = less(work, product(factor, rows[e]))
            drop = (offset + PANEL) // 8 * 8
            tiles[n] = tuple(w[drop:] for w in work)
    return [unit_product(*(jnp.concatenate(part, axis=0) for part in p)) for p in pivots]


def unit_product(pr, pi):
    mag = jnp.sqrt(pr * pr + pi * pi)
    ur = pr / mag
    ui = pi / mag
    n = NB
    while n > 1:
        n //= 2
        ar, ai, br, bi = ur[:n], ui[:n], ur[n:], ui[n:]
        ur, ui = ar * br - ai * bi, ar * bi + ai * br
    return ur, ui


def kernel(
    bands_in, umk_in, coeffs, flux, links,
    cv, perm, u, zm, zp, xp, xm, szm, szp, sxp, sxm, wb, xb,
    acc_a, acc_b, acc_d, left_src, left_dst, down_src, down_dst, corner_src, corner_dst,
    hop, load_sem, send_sem, recv_sem, ez_sem, part_sem, hop_sem,
    bands, umk, index_sem,
):
    i = lax.axis_index("kx")
    j = lax.axis_index("ky")
    ni = lax.axis_size("kx")
    nj = lax.axis_size("ky")
    right = (lax.rem(i + 1, ni), j)
    left = (lax.rem(i + ni - 1, ni), j)
    up = (i, lax.rem(j + 1, nj))
    down = (i, lax.rem(j + nj - 1, nj))
    x_edge = i == ni - 1
    y_edge = j == 0
    edge = jnp.logical_or(x_edge, y_edge)

    def load(t):
        rows = pl.ds(t * TILE, TILE)
        return pltpu.make_async_copy(coeffs.at[:, :, rows, :], cv[t], load_sem.at[t])

    half_tiles = HALF // TILE
    indices = [
        pltpu.make_async_copy(bands_in, bands, index_sem.at[0]),
        pltpu.make_async_copy(umk_in, umk, index_sem.at[1]),
    ]
    for copy in indices:
        copy.start()
    load(half_tiles).start()
    load(0).start()

    def shifted(di, dj):
        return lax.rem(i + di + ni, ni), lax.rem(j + dj + nj, nj)

    in_row = lax.rem(i, GROUP)
    in_column = lax.rem(j, GROUP)
    first_plane = in_column == 0
    last_plane = in_column == GROUP - 1
    wrap_plane = jnp.logical_or(first_plane, last_plane)
    sends_by = (
        first_plane,
        last_plane,
        jnp.logical_and(wrap_plane, in_row == GROUP - 1),
        jnp.logical_and(wrap_plane, in_row == 0),
    )
    relay_of = (shifted(0, -2), shifted(0, 2), shifted(5, 0), shifted(-5, 0))
    is_relay = (
        in_column == GROUP - 2,
        in_column == 1,
        jnp.logical_and(wrap_plane, in_row == 4),
        jnp.logical_and(wrap_plane, in_row == 3),
    )
    relay_from = (shifted(0, 2), shifted(0, -2), shifted(-5, 0), shifted(5, 0))
    relay_to = (up, down, shifted(-4, 0), shifted(4, 0))
    gets_by = (None, None, sends_by[3], sends_by[2])
    gets_from = (None, None, shifted(4, 0), shifted(-4, 0))

    barrier = pltpu.get_barrier_semaphore()
    for device in (right, left, up, down, shifted(1, 1), shifted(-1, -1)):
        pl.semaphore_signal(barrier, inc=1, device_id=device, device_id_type=MESH)
    arrivals = jnp.int32(6)
    for flags, devices in (
        (sends_by, relay_of),
        (is_relay, relay_from),
        ((None, None, *is_relay[2:]), relay_to),
        (gets_by, gets_from),
    ):
        for flag, device in zip(flags, devices, strict=True):
            if flag is None:
                continue
            arrivals = arrivals + jnp.where(flag, 1, 0)

            @pl.when(flag)
            def _(device=device):
                pl.semaphore_signal(barrier, inc=1, device_id=device, device_id_type=MESH)

    for copy in indices:
        copy.wait()
    zero = jnp.int32(0)
    ax = jnp.where(x_edge, umk[0, 0], zero)
    bx = jnp.where(x_edge, umk[0, 1], zero)
    ay = jnp.where(y_edge, umk[1, 0], zero)
    by = jnp.where(y_edge, umk[1, 1], zero)

    size = TILE * TILE
    to = lax.broadcasted_iota(jnp.int32, (size, size), 0)
    take = lax.broadcasted_iota(jnp.int32, (size, size), 1)
    swap = (to % TILE) * TILE + to // TILE
    perm[...] = jnp.where(take == swap, 1.0, 0.0).astype(jnp.bfloat16)

    acc_a[...] = jnp.zeros_like(acc_a)
    acc_b[...] = jnp.zeros_like(acc_b)
    acc_d[...] = jnp.zeros_like(acc_d)

    for t in range(1, half_tiles):
        load(t).start()
        load(t + half_tiles).start()

    def remote(src, dst, stream, c, device):
        return pltpu.make_async_remote_copy(
            src_ref=src, dst_ref=dst, send_sem=send_sem.at[stream, c],
            recv_sem=recv_sem.at[stream, c], device_id=device, device_id_type=MESH,
        )

    def stream_ends(stream, c, special):
        low = pl.ds(c * CHUNK, CHUNK)
        high = pl.ds(HALF + c * CHUNK, CHUNK)
        own, src, dst, device = (
            (low, szm, zm, down),
            (high, szp, zp, up),
            (low, sxp, xp, right),
            (high, sxm, xm, left),
        )[stream]
        source = src.at[low] if special else u.at[own]
        return source, dst.at[low], device

    def slot(stream, c):
        return pl.ds(RELAYED[stream].index(c) * CHUNK, CHUNK)

    def stream_wait(stream, c):
        return remote(*stream_ends(stream, c, False)[:2], stream, c, right)

    def stream_send(stream, c, special, when, first=False):
        source, target, device = stream_ends(stream, c, special)
        if first and stream < 2 and c >= LATE:
            when = jnp.logical_and(when, jnp.logical_not(is_relay[1 - stream]))
        if c not in RELAYED[stream]:

            @pl.when(when)
            def _():
                remote(source, target, stream, c, device).start()

            return

        @pl.when(jnp.logical_and(when, jnp.logical_not(sends_by[stream])))
        def _():
            remote(source, target, stream, c, device).start()

        @pl.when(jnp.logical_and(when, sends_by[stream]))
        def _():
            pltpu.make_async_remote_copy(
                src_ref=source, dst_ref=hop.at[slot(stream, c)],
                send_sem=send_sem.at[stream, c], recv_sem=hop_sem.at[0, c],
                device_id=relay_of[stream], device_id_type=MESH,
            ).start()

    def relay_copy(stream, c):
        source = hop.at[slot(stream, c)]
        target = stream_ends(stream, c, False)[1]
        return pltpu.make_async_remote_copy(
            src_ref=source, dst_ref=target, send_sem=hop_sem.at[1, c],
            recv_sem=recv_sem.at[stream, c], device_id=relay_to[stream],
            device_id_type=MESH,
        )

    def relay_arrival(stream, c):
        rows = hop.at[slot(stream, c)]
        return pltpu.make_async_remote_copy(
            src_ref=rows, dst_ref=rows, send_sem=hop_sem.at[1, c],
            recv_sem=hop_sem.at[0, c], device_id=right, device_id_type=MESH,
        )

    need = (y_edge, x_edge, x_edge, y_edge)

    def gather(t):
        rows = pl.ds(t * TILE, TILE)
        for g in range(ROWS // TILE):
            r, b = divmod(g * TILE, NB)
            parts = [cv[t][r, bands[b + e]] for e in range(TILE)]
            moved = jnp.dot(perm[...], jnp.concatenate(parts, axis=0), preferred_element_type=F32)
            moved = moved.astype(jnp.bfloat16).reshape(TILE, TILE, GY)
            u[rows, pl.ds(g * TILE, TILE), :] = moved

    for t in range(half_tiles):
        for tile, streams in ((t + half_tiles, (1, 3)), (t, (0, 2))):
            load(tile).wait()
            gather(tile)
            if tile == half_tiles:
                pl.semaphore_wait(barrier, arrivals)
            for c in range(t * TILE // CHUNK, (t + 1) * TILE // CHUNK):
                for stream in streams:
                    stream_send(stream, c, False, jnp.logical_not(need[stream]), True)

    def build(dst, count, first, dp, dq):
        shift = lax.rem(GY - dq, GY)

        @pl.loop(0, count // 8)
        def _(c):
            for q in range(8):
                p = c * 8 + q
                row = lax.rem(first + p + dp + GX, GX)
                dst[p] = pltpu.roll(u[row], shift, 1)

    def build_extra(dst, forward, dq):
        shift = lax.rem(GY - dq, GY)
        for e in range(EXTRA):
            row = jnp.where(forward, e, HALF - EXTRA + e)
            dst[HALF + e] = pltpu.roll(u[row], shift, 1)

    def extra(stream, src, dst, device):
        rows = pl.ds(HALF, EXTRA)
        return pltpu.make_async_remote_copy(
            src_ref=src.at[rows], dst_ref=dst.at[rows], send_sem=ez_sem.at[0, stream],
            recv_sem=ez_sem.at[1, stream], device_id=device, device_id_type=MESH,
        )

    @pl.when(y_edge)
    def _():
        build(szm, HALF, 0, -ay, -by)
        for c in range(NCHUNK):
            stream_send(0, c, True, True, True)

    @pl.when(x_edge)
    def _():
        build(szp, HALF, HALF, 0, bx)
        build_extra(szp, ax > 0, bx)
        extra(0, szp, zp, up).start()
        for c in range(NCHUNK):
            stream_send(1, c, True, True, True)
        build(sxp, HALF, 0, ax, bx)
        for c in range(NCHUNK):
            stream_send(2, c, True, True, True)

    @pl.when(y_edge)
    def _():
        build(sxm, HALF, HALF, 0, -by)
        build_extra(sxm, ay < 0, -by)
        extra(1, sxm, xm, left).start()
        for c in range(NCHUNK):
            stream_send(3, c, True, True, True)

    for stream in range(4):

        @pl.when(is_relay[stream])
        def _(stream=stream):
            for c in RELAYED[stream]:
                relay_arrival(stream, c).wait_recv()
                relay_copy(stream, c).start()
            if stream < 2:
                other = 1 - stream
                for c in range(LATE, NCHUNK):
                    stream_send(other, c, False, jnp.logical_not(need[other]))
                    stream_send(other, c, True, need[other])

    build(wb, HALF, HALF, -ay, bx - by)
    build(xb, HALF, HALF, ax, bx - by)

    def diagonal(place, row, count):
        total = None
        for q in range(count):
            source = row + q - ax
            inside = jnp.logical_and(source >= 0, source < HALF)
            target = jnp.where(inside, source - ay, 0)
            target = jnp.where(target < 0, target + HALF + EXTRA, target)
            left_rows = zp[place + q]
            term = dot(jnp.where(inside, left_rows, jnp.zeros_like(left_rows)), xm[target])
            total = term if total is None else total + term
        acc_d[...] += total

    @pl.when(edge)
    def _():
        for c in range(NCHUNK):
            stream_wait(3, c).wait_recv()

    @pl.when(y_edge)
    def _():
        extra(1, sxm, xm, left).wait_recv()

    @pl.when(x_edge)
    def _():
        extra(0, szp, zp, up).wait_recv()
        diagonal(HALF, jnp.where(ax > 0, HALF, -EXTRA), EXTRA)

    def low_terms(c):
        stream_wait(0, c).wait_recv()
        stream_wait(2, c).wait_recv()
        total = None
        for q in range(CHUNK):
            p = c * CHUNK + q
            own = u[p]
            term = dot(
                jnp.concatenate([own, xp[p]], axis=0), jnp.concatenate([zm[p], own], axis=0)
            )
            total = term if total is None else total + term
        acc_a[...] += total

    def high_terms(c):
        stream_wait(1, c).wait_recv()

        @pl.when(jnp.logical_not(edge))
        def _():
            stream_wait(3, c).wait_recv()

        total = None
        for q in range(CHUNK):
            p = c * CHUNK + q
            term = dot(
                jnp.concatenate([zp[p], xb[p]], axis=0), jnp.concatenate([wb[p], xm[p]], axis=0)
            )
            total = term if total is None else total + term
        acc_b[...] += total

        @pl.when(edge)
        def _():
            diagonal(c * CHUNK, c * CHUNK, CHUNK)

    @pl.loop(0, NCHUNK - 1)
    def _(step):
        early, late = RELAYED[0][0], len(RELAYED[0])
        turn = NCHUNK - 1 - late
        c = jnp.where(step < early, step, step + late)
        c = jnp.where(step < turn, c, early + step - turn)
        low_terms(c)
        high_terms(c)

    none = jnp.zeros((NB, NB), F32)

    def table(x, y, d):
        return [jnp.concatenate([x[part], y[part], d[part], none], axis=1) for part in range(2)]

    def part_copy(which):
        src, dst, device = (
            (left_src, left_dst, left),
            (down_src, down_dst, down),
            (corner_src, corner_dst, shifted(-1, -1)),
        )[which]
        return pltpu.make_async_remote_copy(
            src_ref=src, dst_ref=dst, send_sem=part_sem.at[0, which],
            recv_sem=part_sem.at[1, which], device_id=device, device_id_type=MESH,
        )

    low_terms(NCHUNK - 1)
    a = acc_a[...]
    low = table(
        complex_parts(a[ROWS:, ROWS:]),
        complex_parts(a[:ROWS, :ROWS]),
        complex_parts(a[ROWS:, :ROWS]),
    )
    for part in range(2):
        left_src[pl.ds(part * NB, NB), :] = low[part]
    part_copy(0).start()

    high_terms(NCHUNK - 1)

    @pl.when(jnp.logical_not(edge))
    def _():
        acc_d[...] = acc_b[:ROWS, ROWS:]

    b = acc_b[...]
    high = table(
        complex_parts(b[ROWS:, ROWS:]),
        complex_parts(b[:ROWS, :ROWS]),
        complex_parts(acc_d[...]),
    )
    lane = lax.broadcasted_iota(jnp.int32, (NB, 128), 1)
    for part in range(2):
        rows = pl.ds(part * NB, NB)
        down_src[rows, :] = high[part]
        corner_src[rows, :] = jnp.where(lane < NB, left_src[rows, :], high[part])
    part_copy(1).start()
    part_copy(2).start()
    for which in range(3):
        part_copy(which).wait_recv()
    own_tile, next_tile = [], []
    for part in range(2):
        rows = pl.ds(part * NB, NB)
        of_left, of_down, of_corner = left_dst[rows, :], down_dst[rows, :], corner_dst[rows, :]
        other = jnp.where(lane < 2 * NB, left_src[rows, :] + of_down, of_left + of_down)
        other = jnp.where(lane < NB, high[part] + of_left, other)
        own_tile.append(jnp.where(lane < 3 * NB, other, 1.0))
        other = of_corner + jnp.where(lane < NB, of_down, of_left)
        next_tile.append(jnp.where(lane < 2 * NB, other, 1.0))
    unit, unit_next = eliminate((own_tile, next_tile))

    def group(ref, which):
        real, imag = ref
        if which:
            shift = 128 - which * NB
            real, imag = pltpu.roll(real, shift, 1), pltpu.roll(imag, shift, 1)
        return real, imag

    along_x, along_y, along_d = (group(unit, which) for which in range(3))
    y_next = group(unit_next, 1)
    x_next = group(unit_next, 0)
    first = product(product(along_x, y_next), conjugate(along_d))
    second = product(product(along_d, conjugate(x_next)), conjugate(along_y))
    lane = lax.broadcasted_iota(jnp.int32, (1, 128), 1)
    angle = jnp.arctan2(
        jnp.where(lane == 0, first[1], second[1]), jnp.where(lane == 0, first[0], second[0])
    )
    flux[0] = angle[:, :2]
    for part in range(2):
        row = jnp.where(lane == 0, along_x[part], along_y[part])
        row = jnp.where(lane == 2, along_d[part], row)
        links[0, 0, part : part + 1, :] = row[:, :3]

    @pl.loop(0, NCHUNK)
    def _(c):
        for stream in range(4):
            stream_wait(stream, c).wait_send()

    @pl.when(x_edge)
    def _():
        extra(0, szp, zp, up).wait_send()

    @pl.when(y_edge)
    def _():
        extra(1, sxm, xm, left).wait_send()

    for stream in range(4):

        @pl.when(is_relay[stream])
        def _(stream=stream):
            for c in RELAYED[stream]:
                relay_copy(stream, c).wait_send()

    for which in range(3):
        part_copy(which).wait_send()


def per_device(coeffs, bands, umklapp):
    bf16 = jnp.bfloat16
    half = pltpu.VMEM((HALF, ROWS, GY), bf16)
    longer = pltpu.VMEM((HALF + EXTRA, ROWS, GY), bf16)
    flux, links = pl.pallas_call(
        kernel,
        out_shape=(
            jax.ShapeDtypeStruct((1, 1, 2), F32),
            jax.ShapeDtypeStruct((1, 1, 2, 3), F32),
        ),
        in_specs=[
            pl.BlockSpec(memory_space=pltpu.HBM),
            pl.BlockSpec(memory_space=pltpu.HBM),
            pl.BlockSpec(memory_space=pltpu.HBM),
        ],
        out_specs=(pl.BlockSpec(memory_space=pltpu.VMEM),) * 2,
        scratch_shapes=[
            [pltpu.VMEM((*coeffs.shape[2:4], TILE, GY), bf16)] * (GX // TILE),
            pltpu.VMEM((TILE * TILE, TILE * TILE), bf16),
            pltpu.VMEM((GX, ROWS, GY), bf16),
            half, longer, half, longer,
            half, longer, half, longer, half, half,
            pltpu.VMEM((2 * ROWS, 2 * ROWS), F32),
            pltpu.VMEM((2 * ROWS, 2 * ROWS), F32),
            pltpu.VMEM((ROWS, ROWS), F32),
            pltpu.VMEM((ROWS, 128), F32),
            pltpu.VMEM((ROWS, 128), F32),
            pltpu.VMEM((ROWS, 128), F32),
            pltpu.VMEM((ROWS, 128), F32),
            pltpu.VMEM((ROWS, 128), F32),
            pltpu.VMEM((ROWS, 128), F32),
            pltpu.VMEM((max(map(len, RELAYED)) * CHUNK, ROWS, GY), bf16),
            pltpu.SemaphoreType.DMA((GX // TILE,)),
            pltpu.SemaphoreType.DMA((4, NCHUNK)),
            pltpu.SemaphoreType.DMA((4, NCHUNK)),
            pltpu.SemaphoreType.DMA((2, 2)),
            pltpu.SemaphoreType.DMA((2, 3)),
            pltpu.SemaphoreType.DMA((2, NCHUNK)),
            pltpu.SMEM((NB,), jnp.int32),
            pltpu.SMEM((2, 2), jnp.int32),
            pltpu.SemaphoreType.DMA((2,)),
        ],
        compiler_params=pltpu.CompilerParams(
            collective_id=0, has_side_effects=True, vmem_limit_bytes=50 << 20
        ),
    )(*(pltpu.with_memory_space_constraint(v, pltpu.HBM) for v in (bands, umklapp, coeffs[0, 0])))
    return flux, jnp.swapaxes(links, 2, 3)


def solution(mesh):
    in_specs = (P("kx", "ky", None, None, None, None), P(), P())
    out_specs = (P("kx", "ky", None), P("kx", "ky", None, None))
    return jax.shard_map(
        per_device, mesh=mesh, in_specs=in_specs, out_specs=out_specs, check_vma=False
    )
```
